128 devices in a mesh: expert: 64 (over x, y, z), dp: 2 (over core).
Axes of the slice: x: 4, y: 4, z: 4, core: 2. Of those that a mesh axis runs over, the one named last changes fastest.
Arguments:
- patches: bfloat16 [2048, 196, 1024], P(('dp', 'expert')), parts along dimension 0, may hold values from -6 to 6
- visible: int32 [2048, 49], P(('dp', 'expert')), parts along dimension 0, may hold values from 0 to 195, as said below
- routes: int32 [100352, 1], P(('dp', 'expert')), parts along dimension 0, may hold values from 0 to 63; in each aligned block of 784 rows (0 to 783, 784 to 1567, ...) at most 19 rows name the same one
- expert_cap: int32 [128], P('dp'), parts along dimension 0, may hold values from 8 to 19
- norm_gain: float32 [1024], replicated, may hold values from 0.5 to 2
- norm_bias: float32 [1024], replicated, may hold values from -6 to 6
- router: float32 [1024, 64], replicated, may hold values from -0.1875 to 0.1875
- w_in: bfloat16 [64, 1024, 4096], P('expert'), may hold values from -0.1875 to 0.1875
- b_in: float32 [64, 4096], P('expert'), may hold values from -6 to 6
- w_out: bfloat16 [64, 4096, 1024], P('expert'), may hold values from -0.09375 to 0.09375
- b_out: float32 [64, 1024], P('expert'), may hold values from -6 to 6
Outputs:
- layer_out: bfloat16 [100352, 1024], P(('dp', 'expert')), parts along dimension 0
The draws below stay inside these ranges and needn't reach their ends.
There are 2 independent parts, one for each index of `dp`. The reference program is written for one: setup_inputs(seed, part) draws one part's arguments, and reference() takes and returns one part's arrays. A program takes and returns all parts, laid end to end along the dimension named above; an argument that names none is the same for every part. Nothing has to cross between parts.
Inputs may be any that keep to these rules, and one draw needn't show every extreme that they name: `visible`: each row holds 49 different patch indices in increasing order. `routes`: among the tokens of one index of expert no expert is named more than 19 times.
All inputs are finite; a program needn't handle non-finite values.
Results may differ from the reference program's by a relative error of at most 0.005.
Values may be sent and summed in bfloat16 or wider, within the bound.
A program may use at most 128 MiB of HBM per device.

```python
import math
import jax
import jax.numpy as jnp
import numpy as np
from jax import lax

D = 1024
FF = 4096
PATCHES = 196
KEEP = 49
EXPERTS = 64
IMAGES = 1024
TOK_DEV = 784
TOKENS = 50176
CAP = 19
N_EXPERT = 64


def draw_visible(key, part):
    keys = jax.random.split(jax.random.fold_in(key, 7), IMAGES)

    def one_image(k):
        return jnp.sort(jax.random.permutation(k, PATCHES)[:KEEP])
    return jax.vmap(one_image)(keys).astype(jnp.int32)


def with_ends(result, key, smallest, top_value):
    shape = result.shape
    index_at = [jax.random.randint(jax.random.fold_in(key, axis), (), 0, shape[axis]) for axis in range(len(shape))]
    result = result.at[tuple(index_at)].set(smallest)
    longest = shape.index(max(shape))
    index_at[longest] = (index_at[longest] + 1) % shape[longest]
    return result.at[tuple(index_at)].set(top_value)


def block_levels(own_key, shape, cuts, least, high):
    gain, own = 1.0, jax.random.fold_in(own_key, 6)
    for dim, blocks in cuts:
        draws = jnp.exp(jax.random.uniform(jax.random.fold_in(own, dim), (blocks,), jnp.float32, least / len(cuts), high / len(cuts)))
        gain = gain * jnp.repeat(draws, shape[dim] // blocks).reshape([-1 if axis == dim else 1 for axis in range(len(shape))])
    return gain


def assign_block(own_key, own, number, rows, number_of, top, reach, lean):
    order = jax.random.permutation(own_key, number_of)
    heavy_load, common = load_shares(number_of, rows * top, reach, lean, True), load_shares(number_of, rows * top, reach, lean, False)
    places = jnp.arange(number_of)

    def named(tallies, turn):
        used = int((tallies > 0).sum())
        fixed = max(1, used // 4)
        shifted = fixed + (places - fixed + turn * (used - fixed)) % max(1, number_of - fixed)
        return jnp.zeros((number_of,), jnp.int32).at[order[jnp.where(places < fixed, places, shifted)]].set(jnp.asarray(tallies, jnp.int32))

    tallies = jnp.where(number % 4 == 0, named(heavy_load, number // 4), named(common, number - number // 4 - 1))
    mixed = jax.random.permutation(jax.random.fold_in(own, 3), number_of)
    source_of, taker = mixed[0:number_of // 2 * 2:2], mixed[1:number_of // 2 * 2:2]
    slack = jnp.minimum(tallies[source_of] - 1, reach - tallies[taker]) // 2
    slack = jnp.where((source_of == order[0]) | (taker == order[0]) | (tallies[taker] == 0), 0, jnp.maximum(slack, 0))
    shifted = jax.random.randint(jax.random.fold_in(own, 4), (number_of // 2,), 0, 1 << 20) % (slack + 1)
    tallies = tallies.at[source_of].add(-shifted).at[taker].add(shifted)
    labels = jnp.searchsorted(jnp.cumsum(tallies), jnp.arange(rows * top), side="right").astype(jnp.int32)
    table = labels.reshape(top, rows).T
    table = table[jax.random.permutation(jax.random.fold_in(own, 1), rows)]
    turn = jax.random.randint(jax.random.fold_in(own, 2), (rows, 1), 0, top)
    return jnp.take_along_axis(table, (jnp.arange(top)[None, :] + turn) % top, axis=1)


def load_shares(count, total, reach, slope, full):
    loads = [(1 << 20) // math.isqrt(standing ** slope) + 1 for standing in range(1, count + 1)]
    largest = reach if full else min(reach, max(-(-total // count), total * loads[0] // sum(loads)))
    least = 1 if total - largest >= count - 1 else 0
    given, spare = [largest] + [least] * (count - 1), total - largest - least * (count - 1)
    while spare > 0:
        movable = [i for i in range(1, count) if given[i] < largest] or [i for i in range(1, count) if given[i] < reach]
        whole, left = sum([loads[i] for i in movable]), spare
        for i in movable:
            more = min(reach - given[i], max(1, left * loads[i] // whole), spare)
            given[i] = given[i] + more
            spare = spare - more
    return np.array(given)


def gaussian(key, shape, deviation, bound, pieces=(), kind=jnp.bfloat16):
    factor_of = block_levels(key, shape, pieces, -0.22, 0.18) if pieces else 1.0
    result = jax.random.normal(key, shape, jnp.float32) * deviation * factor_of
    return jnp.minimum(jnp.maximum(result, -bound), bound).astype(kind)


def setup_inputs(seed: int = 0, part: int = 0) -> dict:
    splits = jax.random.split(jax.random.key(seed), 12)
    part_keys = jax.random.split(jax.random.fold_in(splits[11], part), 12)
    patches = gaussian(part_keys[0], (IMAGES, PATCHES, D), 1.0, 6.0, ((0, 64),))
    visible = draw_visible(jax.random.fold_in(jax.random.fold_in(splits[11], part), 71), part)
    routes_keys = jax.random.split(jax.random.fold_in(part_keys[2], 1), TOKENS // TOK_DEV)
    routes_turns = jax.random.permutation(jax.random.fold_in(part_keys[2], 3), TOKENS // TOK_DEV)
    routes = jax.vmap(lambda own, number: assign_block(jax.random.fold_in(part_keys[2], 2), own, number, TOK_DEV, EXPERTS, 1, CAP, 2))(routes_keys, routes_turns).reshape((TOKENS, 1))
    expert_cap = with_ends(jax.random.randint(part_keys[3], (EXPERTS,), CAP // 2 - 1, CAP + 1), jax.random.fold_in(part_keys[3], 1), CAP // 2 - 1, CAP).astype(jnp.int32)
    norm_gain = jnp.clip(jnp.exp(jax.random.uniform(splits[4], (D,), jnp.float32, math.log(0.5), math.log(2.0))), 0.5, 2.0)
    norm_bias = gaussian(splits[5], (D,), 1.0, 6.0, (), jnp.float32)
    router = gaussian(splits[6], (D, EXPERTS), D ** -0.5, 0.1875, (), jnp.float32)
    w_in = gaussian(splits[7], (EXPERTS, D, FF), D ** -0.5, 0.1875, ((0, 64),))
    b_in = gaussian(splits[8], (EXPERTS, FF), 1.0, 6.0, ((0, 64),), jnp.float32)
    w_out = gaussian(splits[9], (EXPERTS, FF, D), FF ** -0.5, 0.09375, ((0, 64),))
    b_out = gaussian(splits[10], (EXPERTS, D), 1.0, 6.0, ((0, 64),), jnp.float32)
    return {"patches": patches, "visible": visible, "routes": routes, "expert_cap": expert_cap, "norm_gain": norm_gain, "norm_bias": norm_bias, "router": router, "w_in": w_in, "b_in": b_in, "w_out": w_out, "b_out": b_out}


def reference(patches, visible, routes, expert_cap, norm_gain, norm_bias, router, w_in, b_in, w_out, b_out):
    x = jnp.take_along_axis(patches, visible[:, :, None], axis=1).reshape(TOKENS, D)
    xf = x.astype(jnp.float32)
    mean = lax.optimization_barrier(jnp.mean(xf, axis=1, keepdims=True))
    var = lax.optimization_barrier(jnp.mean((xf - mean) ** 2, axis=1, keepdims=True))
    h = (xf - mean) / jnp.sqrt(var + 1e-06) * norm_gain + norm_bias
    hb = h.astype(jnp.bfloat16)
    chosen = routes[:, 0]
    onehot = (chosen[:, None] == jnp.arange(EXPERTS, dtype=jnp.int32)[None, :]).astype(jnp.int32)
    logits = jnp.dot(h, router, precision=lax.Precision.HIGHEST)
    gate = jax.nn.sigmoid(lax.optimization_barrier(jnp.sum(logits * onehot.astype(jnp.float32), axis=1)))
    blocks = onehot.reshape(N_EXPERT, TOK_DEV, EXPERTS)
    before = (jnp.cumsum(blocks, axis=1) - blocks).reshape(TOKENS, EXPERTS)
    rank = lax.optimization_barrier(jnp.sum(before * onehot, axis=1))
    limit = lax.optimization_barrier(jnp.sum(onehot * expert_cap[None, :], axis=1))
    kept = rank < limit
    source = (jnp.arange(TOKENS, dtype=jnp.int32) // TOK_DEV).astype(jnp.int32)
    rows_each = N_EXPERT * CAP
    dest = jnp.where(kept, chosen * rows_each + source * CAP + rank, EXPERTS * rows_each).astype(jnp.int32)
    buffer = jnp.zeros((EXPERTS * rows_each + 1, D), jnp.bfloat16).at[dest].set(hb)
    buffer = buffer[:-1].reshape(EXPERTS, rows_each, D)

    def expert_step(args):
        rows, first, bias_first, second, bias_second = args
        act = jax.nn.gelu(jnp.dot(rows, first, preferred_element_type=jnp.float32) + bias_first, approximate=True).astype(jnp.bfloat16)
        return (jnp.dot(act, second, preferred_element_type=jnp.float32) + bias_second).astype(jnp.bfloat16)
    results = lax.map(expert_step, (buffer, w_in, b_in, w_out, b_out)).reshape(EXPERTS * rows_each, D)
    picked = results[jnp.minimum(dest, EXPERTS * rows_each - 1)].astype(jnp.float32)
    branch = jnp.where(kept[:, None], gate[:, None] * picked, 0.0)
    return (xf + branch).astype(jnp.bfloat16)
```

```python
import itertools

import jax
import jax.numpy as jnp
from jax import lax
from jax.experimental import pallas as pl
from jax.experimental.pallas import tpu as pltpu
from jax.sharding import PartitionSpec as P

MESH = pl.DeviceIdType.MESH
SIDE = 4
LANES = 128
PLACES = sorted(
    itertools.product(range(SIDE), repeat=3), key=lambda o: (sum(min(d, SIDE - d) for d in o) > 0, (o[0] * 7 + o[1] * 11 + o[2] * 13) % 16)
)
CHUNK = 16


def prep_kernel(
    patches, visible, route_row, route_col, cap_row, cap_col, gain, bias, router,
    blocks, x_out, gate_out, key_out, hb_ref, h_lo, tail,
):
    images, width = patches.shape[1], patches.shape[2]
    keep = visible.shape[1]
    toks = images * keep
    experts = cap_col.shape[0]

    row = lax.broadcasted_iota(jnp.int32, (images, width), 0)

    def pick(k, carry):
        got = patches[visible[0, k]]
        for i in range(1, images):
            got = jnp.where(row == i, patches[visible[i, k]], got)
        start = pl.multiple_of(k * images, images)
        x_out[pl.ds(start, images), :] = got
        xf = got.astype(jnp.float32)
        mean = jnp.sum(xf, axis=1, keepdims=True) * (1.0 / width)
        diff = xf - mean
        var = jnp.sum(diff * diff, axis=1, keepdims=True) * (1.0 / width)
        h = diff * (1.0 / jnp.sqrt(var + 1e-06)) * gain[...] + bias[...]
        hb = h.astype(jnp.bfloat16)
        hb_ref[pl.ds(start, images), :] = hb
        h_lo[pl.ds(start, images), :] = (h - hb.astype(jnp.float32)).astype(jnp.bfloat16)
        return carry

    lax.fori_loop(0, keep, pick, 0)

    def place(shape, dim):
        t = lax.broadcasted_iota(jnp.int32, shape, dim)
        return (t % images) * keep + t // images

    earlier = (place((toks, 1), 0) < place((1, toks), 1)).astype(jnp.bfloat16)
    later = (place((toks, 1), 0) > place((1, toks), 1)).astype(jnp.bfloat16)
    one_row = lax.broadcasted_iota(jnp.int32, (experts, toks), 0) == route_row[...]
    ones = one_row.astype(jnp.float32)
    before = jnp.dot(ones.astype(jnp.bfloat16), earlier, preferred_element_type=jnp.float32)
    rank = jnp.sum(before * ones, axis=0, keepdims=True).astype(jnp.int32)
    limit = jnp.sum(jnp.where(one_row, cap_col[...], 0), axis=0, keepdims=True)
    kept = rank < limit
    chosen = route_row[...]

    hb = hb_ref[...]

    def rows_of(key, count):
        sel = lax.broadcasted_iota(jnp.int32, (count, toks), 0) == key
        return jnp.dot(sel.astype(jnp.bfloat16), hb, preferred_element_type=jnp.float32)

    for part in range(2):
        key = jnp.where(kept & (rank // 8 == part), chosen * 8 + rank % 8, -1)
        got = rows_of(key, experts * 8)
        blocks[:, :, part * width : (part + 1) * width] = got.reshape(experts, 8, width).astype(
            jnp.bfloat16
        )
    key = jnp.where(kept & (rank >= 16), (rank - 16) * experts + chosen, -1)
    got = rows_of(key, experts * 3)
    for r in range(3):
        for j in range(8):
            tail[r, pl.ds(j, experts, stride=8), :] = got[
                r * experts : (r + 1) * experts, j * LANES : (j + 1) * LANES
            ]
        blocks[:, :, 2 * width + r * LANES : 2 * width + (r + 1) * LANES] = (
            tail[r].reshape(experts, 8, LANES).astype(jnp.bfloat16)
        )

    one_col = lax.broadcasted_iota(jnp.int32, (toks, experts), 1) == route_col[...]
    ones_c = one_col.astype(jnp.float32)
    before_c = jnp.dot(later, ones_c.astype(jnp.bfloat16), preferred_element_type=jnp.float32)
    rank_c = jnp.sum(before_c * ones_c, axis=1, keepdims=True).astype(jnp.int32)
    limit_c = jnp.sum(jnp.where(one_col, cap_row[...], 0), axis=1, keepdims=True)
    chosen_c = route_col[...]
    slot = jnp.where(
        rank_c < 8,
        chosen_c * 8 + rank_c,
        jnp.where(
            rank_c < 16,
            experts * 8 + chosen_c * 8 + rank_c - 8,
            experts * rank_c + chosen_c,
        ),
    )
    key_out[...] = jnp.where(rank_c < limit_c, slot, -1)
    r_full = router[...]
    r_hi = r_full.astype(jnp.bfloat16)
    r_lo = (r_full - r_hi.astype(jnp.float32)).astype(jnp.bfloat16)
    logits = (
        jnp.dot(hb, r_lo, preferred_element_type=jnp.float32)
        + jnp.dot(h_lo[...], r_hi, preferred_element_type=jnp.float32)
        + jnp.dot(hb, r_hi, preferred_element_type=jnp.float32)
    )
    score = jnp.sum(logits * ones_c, axis=1, keepdims=True)
    gate_out[...] = 1.0 / (1.0 + jnp.exp(-score))


def exchange_kernel(
    blocks, w_in, b_in, w_out, b_out, back,
    sent, got, made, w1, w2, rows, act, tail, rest,
    load_sem, s_sem, r_sem, ys_sem, yr_sem,
):
    width, hidden = w1.shape
    me = lax.axis_index("expert")
    mx, my, mz = me // (SIDE * SIDE), (me // SIDE) % SIDE, me % SIDE

    def at(o, sign):
        x = (mx + sign * o[0] + SIDE) % SIDE
        y = (my + sign * o[1] + SIDE) % SIDE
        z = (mz + sign * o[2] + SIDE) % SIDE
        return (x * SIDE + y) * SIDE + z

    load = pltpu.make_async_copy(blocks, sent, load_sem.at[0])
    load.start()
    load1 = pltpu.make_async_copy(w_in.at[0], w1, load_sem.at[1])
    load1.start()
    load2 = pltpu.make_async_copy(w_out.at[0], w2, load_sem.at[2])
    load2.start()

    barrier = pltpu.get_barrier_semaphore()
    for o in PLACES[1:]:
        pl.semaphore_signal(barrier, inc=1, device_id={"expert": at(o, 1)}, device_id_type=MESH)
    pl.semaphore_wait(barrier, len(PLACES) - 1)
    load.wait()

    def out_copy(i):
        peer = at(PLACES[i], 1)
        return pltpu.make_async_remote_copy(
            src_ref=sent.at[peer], dst_ref=got.at[i], send_sem=s_sem.at[i], recv_sem=r_sem.at[i],
            device_id={"expert": peer}, device_id_type=MESH,
        )

    def back_copy(i):
        peer = at(PLACES[i], -1)
        return pltpu.make_async_remote_copy(
            src_ref=made.at[i], dst_ref=back.at[me], send_sem=ys_sem.at[i], recv_sem=yr_sem.at[i],
            device_id={"expert": peer}, device_id_type=MESH,
        )

    count = len(PLACES)
    for i in range(1, count):
        out_copy(i).start()
    got[0] = sent[me]
    step = 512
    wide = 256
    for c in range(count // CHUNK):
        lo = c * CHUNK
        for i in range(max(lo, 1), lo + CHUNK):
            out_copy(i).wait_recv()
        half = CHUNK * 8
        for part in range(2):
            piece = got[lo : lo + CHUNK, :, part * width : (part + 1) * width]
            rows[part * half : (part + 1) * half, :] = (
                piece.astype(jnp.float32).reshape(half, width).astype(jnp.bfloat16)
            )
        for r in range(3):
            tail[r] = (
                got[lo : lo + CHUNK, :, 2 * width + r * LANES : 2 * width + (r + 1) * LANES]
                .astype(jnp.float32)
                .reshape(half, LANES)
            )
            for j in range(8):
                at_row = 2 * half + r * CHUNK
                rows[at_row : at_row + CHUNK, j * LANES : (j + 1) * LANES] = tail[
                    r, pl.ds(j, CHUNK, stride=8), :
                ].astype(jnp.bfloat16)
        if c == 0:
            load1.wait()
            load2.wait()

        @pl.loop(0, hidden // step)
        def _(f):
            cols = pl.ds(pl.multiple_of(f * step, step), step)
            v = jnp.dot(rows[...], w1[:, cols], preferred_element_type=jnp.float32) + b_in[:, cols]
            inner = v * (0.7978845608028654 + 0.035677408136300125 * (v * v))
            half_v = 0.5 * v
            act[:, cols] = (half_v + half_v * jnp.tanh(inner)).astype(jnp.bfloat16)

        @pl.loop(0, width // wide)
        def _(n):
            cols = pl.ds(pl.multiple_of(n * wide, wide), wide)
            y = jnp.dot(act[...], w2[:, cols], preferred_element_type=jnp.float32) + b_out[:, cols]
            for part in range(2):
                made[lo : lo + CHUNK, :, pl.ds(pl.multiple_of(part * width + n * wide, wide), wide)] = (
                    y[part * half : (part + 1) * half].reshape(CHUNK, 8, wide).astype(jnp.bfloat16)
                )
            rest[:, cols] = y[2 * half :]

        for r in range(3):
            for j in range(8):
                tail[r, pl.ds(j, CHUNK, stride=8), :] = rest[
                    r * CHUNK : (r + 1) * CHUNK, j * LANES : (j + 1) * LANES
                ]
            made[lo : lo + CHUNK, :, 2 * width + r * LANES : 2 * width + (r + 1) * LANES] = (
                tail[r].reshape(CHUNK, 8, LANES).astype(jnp.bfloat16)
            )
        for i in range(max(lo, 1), lo + CHUNK):
            back_copy(i).start()
        if c == 0:
            own = pltpu.make_async_copy(made.at[0], back.at[me], load_sem.at[3])
            own.start()
    own.wait()
    for i in range(1, count):
        out_copy(i).wait_send()
        back_copy(i).wait_send()
    for i in range(1, count):
        back_copy(i).wait_recv()


def combine_kernel(back, x_ref, gate, key, out, sel, rest, tail, perm, joined):
    experts = back.shape[0]
    toks, width = x_ref.shape
    slots = sel.shape[1]
    images, keep = 16, toks // 16
    sel[...] = (lax.broadcasted_iota(jnp.int32, (toks, slots), 1) == key[...]).astype(jnp.bfloat16)
    t_row = lax.broadcasted_iota(jnp.int32, (1, toks), 1)
    place = (t_row % images) * keep + t_row // images
    perm[...] = (lax.broadcasted_iota(jnp.int32, (toks, toks), 0) == place).astype(jnp.bfloat16)
    for r in range(3):
        tail[r] = (
            back[:, :, 2 * width + r * LANES : 2 * width + (r + 1) * LANES]
            .astype(jnp.float32)
            .reshape(experts * 8, LANES)
        )
        for j in range(8):
            rest[r * experts : (r + 1) * experts, j * LANES : (j + 1) * LANES] = tail[
                r, pl.ds(j, experts, stride=8), :
            ].astype(jnp.bfloat16)
    wide = 256
    for n in range(width // wide):
        cols = slice(n * wide, (n + 1) * wide)
        for part in range(2):
            piece = back[:, :, part * width + n * wide : part * width + (n + 1) * wide]
            joined[part * experts * 8 : (part + 1) * experts * 8, :] = (
                piece.astype(jnp.float32).reshape(experts * 8, wide).astype(jnp.bfloat16)
            )
        joined[2 * experts * 8 :, :] = rest[:, cols]
        f = jnp.dot(sel[...], joined[...], preferred_element_type=jnp.float32)
        total = (x_ref[:, cols].astype(jnp.float32) + gate[...] * f).astype(jnp.bfloat16)
        out[:, cols] = jnp.dot(perm[...], total, preferred_element_type=jnp.float32).astype(
            jnp.bfloat16
        )


def per_device(
    patches, visible, routes, expert_cap, norm_gain, norm_bias, router, w_in, b_in, w_out, b_out
):
    images, _, width = patches.shape
    keep = visible.shape[1]
    toks = images * keep
    experts = expert_cap.shape[0]
    hidden = w_in.shape[2]
    by_patch = jnp.transpose(patches, (1, 0, 2))
    route = routes.reshape(images, keep).T.reshape(1, toks)
    vmem = pl.BlockSpec(memory_space=pltpu.VMEM)
    smem = pl.BlockSpec(memory_space=pltpu.SMEM)
    any_ = pl.BlockSpec(memory_space=pl.ANY)
    blk = (experts, 8, 2 * width + 3 * LANES)
    half = CHUNK * 8
    sent, x, gate, key = pl.pallas_call(
        prep_kernel,
        out_shape=(
            jax.ShapeDtypeStruct(blk, jnp.bfloat16),
            jax.ShapeDtypeStruct((toks, width), jnp.bfloat16),
            jax.ShapeDtypeStruct((toks, 1), jnp.float32),
            jax.ShapeDtypeStruct((toks, 1), jnp.int32),
        ),
        in_specs=[vmem, smem] + [vmem] * 7,
        out_specs=(vmem,) * 4,
        scratch_shapes=[
            pltpu.VMEM((toks, width), jnp.bfloat16),
            pltpu.VMEM((toks, width), jnp.bfloat16),
            pltpu.VMEM((3, experts * 8, LANES), jnp.float32),
        ],
        compiler_params=pltpu.CompilerParams(vmem_limit_bytes=56 * 2**20),
        name="prep",
    )(
        by_patch, visible, route, route.reshape(toks, 1), expert_cap.reshape(1, experts),
        expert_cap.reshape(experts, 1), norm_gain.reshape(1, width), norm_bias.reshape(1, width), router,
    )
    back = pl.pallas_call(
        exchange_kernel,
        out_shape=jax.ShapeDtypeStruct(blk, jnp.bfloat16),
        in_specs=[any_, any_, vmem, any_, vmem],
        out_specs=any_,
        scratch_shapes=[
            pltpu.VMEM(blk, jnp.bfloat16),
            pltpu.VMEM(blk, jnp.bfloat16),
            pltpu.VMEM(blk, jnp.bfloat16),
            pltpu.VMEM((width, hidden), jnp.bfloat16),
            pltpu.VMEM((hidden, width), jnp.bfloat16),
            pltpu.VMEM((CHUNK * 19, width), jnp.bfloat16),
            pltpu.VMEM((CHUNK * 19, hidden), jnp.bfloat16),
            pltpu.VMEM((3, half, LANES), jnp.float32),
            pltpu.VMEM((CHUNK * 3, width), jnp.float32),
            pltpu.SemaphoreType.DMA((4,)),
            pltpu.SemaphoreType.DMA((experts,)),
            pltpu.SemaphoreType.DMA((experts,)),
            pltpu.SemaphoreType.DMA((experts,)),
            pltpu.SemaphoreType.DMA((experts,)),
        ],
        compiler_params=pltpu.CompilerParams(
            collective_id=0, has_side_effects=True, vmem_limit_bytes=56 * 2**20
        ),
        name="exchange",
    )(sent, w_in, b_in, w_out, b_out)
    return pl.pallas_call(
        combine_kernel,
        out_shape=jax.ShapeDtypeStruct((toks, width), jnp.bfloat16),
        in_specs=[vmem] * 4,
        out_specs=vmem,
        scratch_shapes=[
            pltpu.VMEM((toks, experts * 19), jnp.bfloat16),
            pltpu.VMEM((experts * 3, width), jnp.bfloat16),
            pltpu.VMEM((3, experts * 8, LANES), jnp.float32),
            pltpu.VMEM((toks, toks), jnp.bfloat16),
            pltpu.VMEM((experts * 19, 256), jnp.bfloat16),
        ],
        compiler_params=pltpu.CompilerParams(vmem_limit_bytes=56 * 2**20),
        name="combine",
    )(back, x, gate, key)


def solution(mesh):
    return jax.shard_map(
        per_device,
        mesh=mesh,
        in_specs=(
            P(("dp", "expert"), None, None),
            P(("dp", "expert"), None),
            P(("dp", "expert"), None),
            P("dp"),
            P(),
            P(),
            P(),
            P("expert", None, None),
            P("expert", None),
            P("expert", None, None),
            P("expert", None),
        ),
        out_specs=P(("dp", "expert"), None),
        check_vma=False,
    )
```

```python
import itertools

import jax
import jax.numpy as jnp
from jax import lax
from jax.experimental import pallas as pl
from jax.experimental.pallas import tpu as pltpu
from jax.sharding import PartitionSpec as P

MESH = pl.DeviceIdType.MESH
SIDE = 4
LANES = 128
PLACES = sorted(
    itertools.product(range(SIDE), repeat=3),
    key=lambda o: (o != (0, 0, 0), (o[0] * 7 + o[1] * 11 + o[2] * 13) % 16),
)
CHUNK = 16
HIGH = 16 * CHUNK
SLOTS = 19 * CHUNK
CHUNKS = len(PLACES) // CHUNK
F32 = jnp.float32
BF16 = jnp.bfloat16


def iota(shape, dim):
    return lax.broadcasted_iota(jnp.int32, shape, dim)


def layer_kernel(
    patches, visible, route, cap, gain, bias, router, w_in, b_in, w_out, b_out, out,
    store, sent, got, made, back, w1, w2, rows, act, tail, rest, picked, hb, ordered, gate, sel, total,
    load_sem, s_sem, r_sem, ys_sem, yr_sem,
):
    images, width = store.shape[1], store.shape[2]
    keep = visible.shape[1]
    toks = images * keep
    experts = cap.shape[1]
    hidden = w1.shape[1]
    me = lax.axis_index("expert")
    mx, my, mz = me // (SIDE * SIDE), (me // SIDE) % SIDE, me % SIDE

    def at(o, sign):
        x = (mx + sign * o[0] + SIDE) % SIDE
        y = (my + sign * o[1] + SIDE) % SIDE
        z = (mz + sign * o[2] + SIDE) % SIDE
        return (x * SIDE + y) * SIDE + z

    load = pltpu.make_async_copy(patches, store, load_sem.at[0])
    load.start()
    barrier = pltpu.get_barrier_semaphore()
    for o in PLACES[1:]:
        pl.semaphore_signal(barrier, inc=1, device_id={"expert": at(o, 1)}, device_id_type=MESH)

    def place(shape, dim):
        t = iota(shape, dim)
        return (t % images) * keep + t // images

    def slot_of(block, rank):
        j = block % CHUNK
        inside = jnp.where(
            rank < 8,
            j * 8 + rank,
            jnp.where(rank < 16, 8 * CHUNK + j * 8 + rank - 8, rank * CHUNK + j),
        )
        return (block // CHUNK) * SLOTS + inside

    block_col = jnp.zeros((experts, 1), jnp.int32)
    block_row = jnp.zeros((1, experts), jnp.int32)
    for i, o in enumerate(PLACES):
        where = at(o, 1)
        block_col = jnp.where(iota((experts, 1), 0) == where, i, block_col)
        block_row = jnp.where(iota((1, experts), 1) == where, i, block_row)

    diag = iota((experts, experts), 0) == iota((experts, experts), 1)
    cap_col = jnp.sum(jnp.where(diag, cap[...], 0), axis=1, keepdims=True)
    route_b = jnp.broadcast_to(route[...], (8, toks)).astype(F32).astype(BF16)
    to_picked = (iota((toks, 1), 0) == place((1, toks), 1)).astype(BF16)
    route_p = jnp.dot(route_b, to_picked, preferred_element_type=F32)[:1].astype(jnp.int32)
    one_row = iota((experts, toks), 0) == route_p
    ones = one_row.astype(F32)
    earlier = (place((toks, 1), 0) < place((1, toks), 1)).astype(BF16)
    before = jnp.dot(ones.astype(BF16), earlier, preferred_element_type=F32)
    rank = jnp.sum(before * ones, axis=0, keepdims=True).astype(jnp.int32)
    limit = jnp.sum(jnp.where(one_row, cap_col, 0), axis=0, keepdims=True)
    block = jnp.sum(jnp.where(one_row, block_col, 0), axis=0, keepdims=True)
    key = jnp.where(rank < limit, slot_of(block, rank), -1)

    load.wait()
    load1 = pltpu.make_async_copy(w_in.at[0], w1, load_sem.at[1])
    load1.start()
    load2 = pltpu.make_async_copy(w_out.at[0], w2, load_sem.at[2])
    load2.start()

    row = iota((images, width), 0)

    def pick(k, carry):
        val = store[visible[0, k]]
        for i in range(1, images):
            val = jnp.where(row == i, store[visible[i, k]], val)
        picked[pl.ds(pl.multiple_of(k * images, images), images), :] = val
        return carry

    lax.fori_loop(0, keep, pick, 0, unroll=7)

    def normed(xf):
        mean = jnp.sum(xf, axis=1, keepdims=True) * (1.0 / width)
        diff = xf - mean
        var = jnp.sum(diff * diff, axis=1, keepdims=True) * (1.0 / width)
        return diff * (1.0 / jnp.sqrt(var + 1e-06)) * gain[...] + bias[...]

    def norm(k, carry):
        span = pl.ds(pl.multiple_of(k * images, images), images)
        hb[span, :] = normed(picked[span, :].astype(F32)).astype(BF16)
        return carry

    lax.fori_loop(0, keep, norm, 0, unroll=7)

    def out_copy(i):
        return pltpu.make_async_remote_copy(
            src_ref=sent.at[i], dst_ref=got.at[i], send_sem=s_sem.at[i], recv_sem=r_sem.at[i],
            device_id={"expert": at(PLACES[i], 1)}, device_id_type=MESH,
        )

    def back_copy(i):
        return pltpu.make_async_remote_copy(
            src_ref=made.at[i], dst_ref=back.at[i], send_sem=ys_sem.at[i], recv_sem=yr_sem.at[i],
            device_id={"expert": at(PLACES[i], -1)}, device_id_type=MESH,
        )

    half = 8 * CHUNK

    def put(ref, lo, y, cols, start):
        wide = y.shape[1]
        for part in range(2):
            lanes = pl.ds(pl.multiple_of(part * width + start, wide), wide)
            ref[lo : lo + CHUNK, :, lanes] = (
                y[part * half : (part + 1) * half].reshape(CHUNK, 8, wide).astype(BF16)
            )
        rest[:, cols] = y[HIGH:]

    def put_rest(ref, lo):
        for r in range(3):
            for j in range(8):
                tail[r, pl.ds(j, CHUNK, stride=8), :] = rest[
                    r * CHUNK : (r + 1) * CHUNK, j * LANES : (j + 1) * LANES
                ]
            lanes = slice(2 * width + r * LANES, 2 * width + (r + 1) * LANES)
            ref[lo : lo + CHUNK, :, lanes] = tail[r].reshape(CHUNK, 8, LANES).astype(BF16)

    def take(ref, lo):
        for part in range(2):
            piece = ref[lo : lo + CHUNK, :, part * width : (part + 1) * width]
            rows[part * half : (part + 1) * half, :] = (
                piece.astype(F32).reshape(half, width).astype(BF16)
            )
        for r in range(3):
            lanes = slice(2 * width + r * LANES, 2 * width + (r + 1) * LANES)
            tail[r] = ref[lo : lo + CHUNK, :, lanes].astype(F32).reshape(half, LANES)
            for j in range(8):
                first = HIGH + r * CHUNK
                rows[first : first + CHUNK, j * LANES : (j + 1) * LANES] = tail[
                    r, pl.ds(j, CHUNK, stride=8), :
                ].astype(BF16)

    wide = 256
    for c in range(CHUNKS):
        lo = c * CHUNK
        chosen = (iota((SLOTS, toks), 0) + c * SLOTS == key).astype(BF16)
        for n in range(width // wide):
            cols = slice(n * wide, (n + 1) * wide)
            y = jnp.dot(chosen, hb[:, cols], preferred_element_type=F32)
            put(sent, lo, y, cols, n * wide)
        put_rest(sent, lo)
        if c == 0:
            pl.semaphore_wait(barrier, len(PLACES) - 1)
        for i in range(max(lo, 1), lo + CHUNK):
            out_copy(i).start()
        if c == 0:
            got[0] = sent[0]

    to_own = (place((1, toks), 1) == iota((toks, 1), 0)).astype(BF16)
    for n in range(width // wide):
        cols = slice(n * wide, (n + 1) * wide)
        ordered[:, cols] = jnp.dot(to_own, picked[:, cols], preferred_element_type=F32).astype(BF16)
    eye = (iota((toks, 1), 0) == iota((1, toks), 1)).astype(BF16)
    route_c = lax.dot_general(
        eye, route_b, (((1,), (1,)), ((), ())), preferred_element_type=F32
    )[:, :1].astype(jnp.int32)
    one_col = iota((toks, experts), 1) == route_c
    ones_c = one_col.astype(F32)
    lower = (iota((toks, 1), 0) > iota((1, toks), 1)).astype(BF16)
    before_c = jnp.dot(lower, ones_c.astype(BF16), preferred_element_type=F32)
    rank_c = jnp.sum(before_c * ones_c, axis=1, keepdims=True).astype(jnp.int32)
    limit_c = jnp.sum(jnp.where(one_col, cap[...], 0), axis=1, keepdims=True)
    block_c = jnp.sum(jnp.where(one_col, block_row, 0), axis=1, keepdims=True)
    key_c = jnp.where(rank_c < limit_c, slot_of(block_c, rank_c), -1)
    for c in range(CHUNKS):
        sel[c] = (iota((toks, SLOTS), 1) + c * SLOTS == key_c).astype(BF16)

    r_full = router[...]
    r_hi = r_full.astype(BF16)
    r_lo = (r_full - r_hi.astype(F32)).astype(BF16)

    def product(a, b):
        return lax.dot_general(a, b, (((1,), (1,)), ((), ())), preferred_element_type=F32)

    group = 7 * images
    for g in range(toks // group):
        span = slice(g * group, (g + 1) * group)
        h = normed(ordered[span, :].astype(F32))
        h_hi = h.astype(BF16)
        h_lo = (h - h_hi.astype(F32)).astype(BF16)
        logits = product(h_hi, r_lo) + product(h_lo, r_hi) + product(h_hi, r_hi)
        score = jnp.sum(logits * ones_c[span], axis=1, keepdims=True)
        gate[span, :] = jnp.broadcast_to(1.0 / (1.0 + jnp.exp(-score)), (group, LANES))

    step = 512

    def gather_back(c):
        lo = c * CHUNK
        for i in range(max(lo, 1), lo + CHUNK):
            back_copy(i).wait_recv()
        take(back, lo)
        for n in range(width // wide):
            cols = slice(n * wide, (n + 1) * wide)
            part = jnp.dot(sel[c], rows[:, cols], preferred_element_type=F32)
            if c > 0:
                part = part + total[:, cols]
            if c < CHUNKS - 1:
                total[:, cols] = part
            else:
                out[:, cols] = (ordered[:, cols].astype(F32) + gate[:, :1] * part).astype(BF16)

    for c in range(CHUNKS):
        lo = c * CHUNK
        for i in range(max(lo, 1), lo + CHUNK):
            out_copy(i).wait_recv()
        take(got, lo)
        if c == 0:
            load1.wait()
            load2.wait()

        @pl.loop(0, hidden // step)
        def _(f):
            cols = pl.ds(pl.multiple_of(f * step, step), step)
            v = jnp.dot(rows[...], w1[:, cols], preferred_element_type=F32) + b_in[:, cols]
            inner = v * (0.7978845608028654 + 0.035677408136300125 * (v * v))
            half_v = 0.5 * v
            act[:, cols] = (half_v + half_v * jnp.tanh(inner)).astype(BF16)

        @pl.loop(0, width // wide)
        def _(n):
            start = n * wide
            cols = pl.ds(pl.multiple_of(start, wide), wide)
            y = jnp.dot(act[...], w2[:, cols], preferred_element_type=F32) + b_out[:, cols]
            put(made, lo, y, cols, start)

        put_rest(made, lo)
        for i in range(max(lo, 1), lo + CHUNK):
            back_copy(i).start()
        if c == 0:
            back[0] = made[0]
        if c >= 2:
            gather_back(c - 2)
    for i in range(1, len(PLACES)):
        out_copy(i).wait_send()
    gather_back(CHUNKS - 2)
    gather_back(CHUNKS - 1)
    for i in range(1, len(PLACES)):
        back_copy(i).wait_send()


def per_device(
    patches, visible, routes, expert_cap, norm_gain, norm_bias, router, w_in, b_in, w_out, b_out
):
    images, _, width = patches.shape
    toks = images * visible.shape[1]
    experts = expert_cap.shape[0]
    hidden = w_in.shape[2]
    by_patch = jnp.transpose(patches, (1, 0, 2))
    vmem = pl.BlockSpec(memory_space=pltpu.VMEM)
    smem = pl.BlockSpec(memory_space=pltpu.SMEM)
    any_ = pl.BlockSpec(memory_space=pl.ANY)
    blk = (experts, 8, 2 * width + 3 * LANES)
    dma = pltpu.SemaphoreType.DMA
    return pl.pallas_call(
        layer_kernel,
        out_shape=jax.ShapeDtypeStruct((toks, width), BF16),
        in_specs=[any_, smem] + [vmem] * 5 + [any_, vmem, any_, vmem],
        out_specs=vmem,
        scratch_shapes=[
            pltpu.VMEM(by_patch.shape, BF16),
            pltpu.VMEM(blk, BF16),
            pltpu.VMEM(blk, BF16),
            pltpu.VMEM(blk, BF16),
            pltpu.VMEM(blk, BF16),
            pltpu.VMEM((width, hidden), BF16),
            pltpu.VMEM((hidden, width), BF16),
            pltpu.VMEM((SLOTS, width), BF16),
            pltpu.VMEM((SLOTS, hidden), BF16),
            pltpu.VMEM((3, 8 * CHUNK, LANES), F32),
            pltpu.VMEM((3 * CHUNK, width), F32),
            pltpu.VMEM((toks, width), BF16),
            pltpu.VMEM((toks, width), BF16),
            pltpu.VMEM((toks, width), BF16),
            pltpu.VMEM((toks, LANES), F32),
            pltpu.VMEM((CHUNKS, toks, SLOTS), BF16),
            pltpu.VMEM((toks, width), F32),
            dma((3,)),
            dma((experts,)),
            dma((experts,)),
            dma((experts,)),
            dma((experts,)),
        ],
        compiler_params=pltpu.CompilerParams(
            collective_id=0, has_side_effects=True, vmem_limit_bytes=63 * 2**20
        ),
        name="layer",
    )(
        by_patch, visible, routes.reshape(1, toks), expert_cap.reshape(1, experts),
        norm_gain.reshape(1, width), norm_bias.reshape(1, width), router.T, w_in, b_in, w_out, b_out,
    )


def solution(mesh):
    return jax.shard_map(
        per_device,
        mesh=mesh,
        in_specs=(
            P(("dp", "expert"), None, None),
            P(("dp", "expert"), None),
            P(("dp", "expert"), None),
            P("dp"),
            P(),
            P(),
            P(),
            P("expert", None, None),
            P("expert", None),
            P("expert", None, None),
            P("expert", None),
        ),
        out_specs=P(("dp", "expert"), None),
        check_vma=False,
    )
```

```python
import jax
import jax.numpy as jnp
from jax import lax
from jax.experimental import pallas as pl
from jax.experimental.pallas import tpu as pltpu
from jax.sharding import PartitionSpec as P

MESH = pl.DeviceIdType.MESH
SIDE = 4
LANES = 128
PARTNERS = SIDE**3
TURN = 37
BACKTURN = 45
CHUNK = 16
HIGH = 16 * CHUNK
SLOTS = 19 * CHUNK
CHUNKS = PARTNERS // CHUNK
F32 = jnp.float32
BF16 = jnp.bfloat16


def iota(shape, dim):
    return lax.broadcasted_iota(jnp.int32, shape, dim)


def layer_kernel(
    patches, visible, route, cap, gain, bias, router, w_in, b_in, w_out, b_out, out,
    store, sent, got, made, back, w1, w2, rows, act, even, odd, tail, picked, hb, ordered, gate, sel,
    total, load_sem, s_sem, r_sem, ys_sem, yr_sem,
):
    images, width = store.shape[1], store.shape[2]
    keep = visible.shape[1]
    toks = images * keep
    experts = cap.shape[1]
    hidden = w1.shape[1]
    me = lax.axis_index("expert")
    mx, my, mz = me // (SIDE * SIDE), (me // SIDE) % SIDE, me % SIDE

    def partner(i, sign):
        code = (i * TURN) % PARTNERS
        x = (mx + sign * (code // (SIDE * SIDE)) + SIDE) % SIDE
        y = (my + sign * ((code // SIDE) % SIDE) + SIDE) % SIDE
        z = (mz + sign * (code % SIDE) + SIDE) % SIDE
        return (x * SIDE + y) * SIDE + z

    load = pltpu.make_async_copy(patches, store, load_sem.at[0])
    load.start()
    barrier = pltpu.get_barrier_semaphore()
    for i in range(1, PARTNERS):
        pl.semaphore_signal(barrier, inc=1, device_id={"expert": partner(i, 1)}, device_id_type=MESH)

    def place(shape, dim):
        t = iota(shape, dim)
        return (t % images) * keep + t // images

    def slot_of(block, rank):
        j = block % CHUNK
        inside = jnp.where(
            rank < 8,
            j * 8 + rank,
            jnp.where(rank < 16, 8 * CHUNK + j * 8 + rank - 8, rank * CHUNK + j),
        )
        return (block // CHUNK) * SLOTS + inside

    def block_of(expert):
        x = (expert // (SIDE * SIDE) - mx + SIDE) % SIDE
        y = ((expert // SIDE) % SIDE - my + SIDE) % SIDE
        z = (expert % SIDE - mz + SIDE) % SIDE
        return (((x * SIDE + y) * SIDE + z) * BACKTURN) % PARTNERS

    diag = iota((experts, experts), 0) == iota((experts, experts), 1)
    cap_col = jnp.sum(jnp.where(diag, cap[...], 0), axis=1, keepdims=True)
    route_b = jnp.broadcast_to(route[...], (8, toks)).astype(F32).astype(BF16)
    to_picked = (iota((toks, 1), 0) == place((1, toks), 1)).astype(BF16)
    route_p = jnp.dot(route_b, to_picked, preferred_element_type=F32)[:1].astype(jnp.int32)
    one_row = iota((experts, toks), 0) == route_p
    ones = one_row.astype(F32)
    earlier = (place((toks, 1), 0) < place((1, toks), 1)).astype(BF16)
    before = jnp.dot(ones.astype(BF16), earlier, preferred_element_type=F32)
    rank = jnp.sum(before * ones, axis=0, keepdims=True).astype(jnp.int32)
    limit = jnp.sum(jnp.where(one_row, cap_col, 0), axis=0, keepdims=True)
    key = jnp.where(rank < limit, slot_of(block_of(route_p), rank), -1)

    load.wait()
    load1 = pltpu.make_async_copy(w_in.at[0], w1, load_sem.at[1])
    load1.start()
    load2 = pltpu.make_async_copy(w_out.at[0], w2, load_sem.at[2])
    load2.start()

    row = iota((images, width), 0)

    def pick(k, carry):
        val = store[visible[0, k]]
        for i in range(1, images):
            val = jnp.where(row == i, store[visible[i, k]], val)
        picked[pl.ds(pl.multiple_of(k * images, images), images), :] = val
        return carry

    lax.fori_loop(0, keep, pick, 0, unroll=7)

    def normed(xf):
        mean = jnp.sum(xf, axis=1, keepdims=True) * (1.0 / width)
        diff = xf - mean
        var = jnp.sum(diff * diff, axis=1, keepdims=True) * (1.0 / width)
        return diff * (1.0 / jnp.sqrt(var + 1e-06)) * gain[...] + bias[...]

    def norm(k, carry):
        span = pl.ds(pl.multiple_of(k * images, images), images)
        hb[span, :] = normed(picked[span, :].astype(F32)).astype(BF16)
        return carry

    lax.fori_loop(0, keep, norm, 0, unroll=7)

    def out_copy(i):
        return pltpu.make_async_remote_copy(
            src_ref=sent.at[i], dst_ref=got.at[i], send_sem=s_sem.at[i], recv_sem=r_sem.at[i],
            device_id={"expert": partner(i, 1)}, device_id_type=MESH,
        )

    def back_copy(i):
        return pltpu.make_async_remote_copy(
            src_ref=made.at[i], dst_ref=back.at[i], send_sem=ys_sem.at[i], recv_sem=yr_sem.at[i],
            device_id={"expert": partner(i, -1)}, device_id_type=MESH,
        )

    half = 8 * CHUNK

    def each(c, act_on):
        @pl.when(c > 0)
        def _():
            act_on(c * CHUNK)

        for i in range(1, CHUNK):
            act_on(c * CHUNK + i)

    def put(ref, lo, y):
        span = pl.ds(lo, CHUNK)
        for part in range(2):
            ref[span, :, part * width : (part + 1) * width] = (
                y[part * half : (part + 1) * half].reshape(CHUNK, 8, width).astype(BF16)
            )
        for r in range(3):
            first = HIGH + r * CHUNK
            for j in range(8):
                tail[r, pl.ds(j, CHUNK, stride=8), :] = y[
                    first : first + CHUNK, j * LANES : (j + 1) * LANES
                ]
            lanes = slice(2 * width + r * LANES, 2 * width + (r + 1) * LANES)
            ref[span, :, lanes] = tail[r].reshape(CHUNK, 8, LANES).astype(BF16)

    def take(ref, lo):
        span = pl.ds(lo, CHUNK)
        for part in range(2):
            piece = ref[span, :, part * width : (part + 1) * width]
            rows[part * half : (part + 1) * half, :] = (
                piece.astype(F32).reshape(half, width).astype(BF16)
            )
        for r in range(3):
            lanes = slice(2 * width + r * LANES, 2 * width + (r + 1) * LANES)
            tail[r] = ref[span, :, lanes].astype(F32).reshape(half, LANES)
            for j in range(8):
                first = HIGH + r * CHUNK
                rows[first : first + CHUNK, j * LANES : (j + 1) * LANES] = tail[
                    r, pl.ds(j, CHUNK, stride=8), :
                ].astype(BF16)

    @pl.loop(0, CHUNKS)
    def _(c):
        chosen = (iota((SLOTS, toks), 0) + c * SLOTS == key).astype(BF16)
        put(sent, c * CHUNK, jnp.dot(chosen, hb[...], preferred_element_type=F32))

        @pl.when(c == 0)
        def _():
            pl.semaphore_wait(barrier, PARTNERS - 1)
            got[0] = sent[0]

        each(c, lambda i: out_copy(i).start())

    total[...] = jnp.zeros_like(total)
    to_own = (place((1, toks), 1) == iota((toks, 1), 0)).astype(BF16)
    ordered[...] = jnp.dot(to_own, picked[...], preferred_element_type=F32).astype(BF16)
    eye = (iota((toks, 1), 0) == iota((1, toks), 1)).astype(BF16)

    def product(a, b):
        return lax.dot_general(a, b, (((1,), (1,)), ((), ())), preferred_element_type=F32)

    route_c = product(eye, route_b)[:, :1].astype(jnp.int32)
    one_col = iota((toks, experts), 1) == route_c
    ones_c = one_col.astype(F32)
    lower = (iota((toks, 1), 0) > iota((1, toks), 1)).astype(BF16)
    before_c = jnp.dot(lower, ones_c.astype(BF16), preferred_element_type=F32)
    rank_c = jnp.sum(before_c * ones_c, axis=1, keepdims=True).astype(jnp.int32)
    limit_c = jnp.sum(jnp.where(one_col, cap[...], 0), axis=1, keepdims=True)
    block_c = jnp.sum(
        jnp.where(one_col, block_of(iota((1, experts), 1)), 0), axis=1, keepdims=True
    )
    key_c = jnp.where(rank_c < limit_c, slot_of(block_c, rank_c), -1)
    for c in range(CHUNKS):
        sel[c] = (iota((toks, SLOTS), 1) + c * SLOTS == key_c).astype(BF16)

    r_full = router[...]
    r_hi = r_full.astype(BF16)
    r_lo = (r_full - r_hi.astype(F32)).astype(BF16)
    group = 7 * images
    for g in range(toks // group):
        span = slice(g * group, (g + 1) * group)
        h = normed(ordered[span, :].astype(F32))
        h_hi = h.astype(BF16)
        h_lo = (h - h_hi.astype(F32)).astype(BF16)
        logits = product(h_hi, r_lo) + product(h_lo, r_hi) + product(h_hi, r_hi)
        score = jnp.sum(logits * ones_c[span], axis=1, keepdims=True)
        gate[span, :] = jnp.broadcast_to(1.0 / (1.0 + jnp.exp(-score)), (group, LANES))

    step = 1024
    last = hidden - step

    def enter(f, ref):
        ref[...] = jnp.dot(rows[...], w1[:, f : f + step], preferred_element_type=F32)

    def bend(f, ref):
        v = ref[...] + b_in[:, f : f + step]
        inner = v * (0.7978845608028654 + 0.035677408136300125 * (v * v))
        half_v = 0.5 * v
        act[:, f : f + step] = (half_v + half_v * jnp.tanh(inner)).astype(BF16)

    load1.wait()
    load2.wait()

    @pl.loop(0, CHUNKS)
    def _(c):
        each(c, lambda i: out_copy(i).wait_recv())
        take(got, c * CHUNK)
        spare = (even, odd)
        enter(0, even)
        for n in range(1, hidden // step):
            enter(n * step, spare[n % 2])
            bend((n - 1) * step, spare[(n - 1) % 2])
        y = jnp.dot(act[:, :last], w2[:last, :], preferred_element_type=F32)
        bend(last, spare[(hidden // step - 1) % 2])
        y = y + jnp.dot(act[:, last:], w2[last:, :], preferred_element_type=F32)
        put(made, c * CHUNK, y + b_out[...])
        each(c, lambda i: back_copy(i).start())

        @pl.when(c == 0)
        def _():
            back[0] = made[0]

        @pl.when(c >= 2)
        def _():
            each(c - 2, lambda i: back_copy(i).wait_recv())
            take(back, (c - 2) * CHUNK)
            total[...] += jnp.dot(sel[c - 2], rows[...], preferred_element_type=F32)

    @pl.loop(1, PARTNERS)
    def _(i):
        out_copy(i).wait_send()

    c = CHUNKS - 2
    each(c, lambda i: back_copy(i).wait_recv())
    take(back, c * CHUNK)
    total[...] += jnp.dot(sel[c], rows[...], preferred_element_type=F32)
    c = CHUNKS - 1
    each(c, lambda i: back_copy(i).wait_recv())
    take(back, c * CHUNK)
    wide = width // 2
    writes = []
    for n in range(2):
        cols = slice(n * wide, (n + 1) * wide)
        part = total[:, cols] + jnp.dot(sel[c], rows[:, cols], preferred_element_type=F32)
        hb[:, cols] = (ordered[:, cols].astype(F32) + gate[:, :1] * part).astype(BF16)
        writes.append(pltpu.make_async_copy(hb.at[:, cols], out.at[:, cols], load_sem.at[n]))
        writes[-1].start()

    @pl.loop(1, PARTNERS)
    def _(i):
        back_copy(i).wait_send()

    for write in writes:
        write.wait()


def finish_kernel(src, out, buf, in_sem, out_sem):
    rows = src.shape[0]
    size = rows // in_sem.shape[0]
    pieces = [pl.ds(n * size, size) for n in range(in_sem.shape[0])]
    loads = [pltpu.make_async_copy(src.at[p], buf.at[p], in_sem.at[n]) for n, p in enumerate(pieces)]
    stores = [pltpu.make_async_copy(buf.at[p], out.at[p], out_sem.at[n]) for n, p in enumerate(pieces)]
    for copy in loads:
        copy.start()
    for n, copy in enumerate(stores):
        loads[n].wait()
        copy.start()
    for copy in stores:
        copy.wait()


def per_device(
    patches, visible, routes, expert_cap, norm_gain, norm_bias, router, w_in, b_in, w_out, b_out
):
    images, _, width = patches.shape
    toks = images * visible.shape[1]
    experts = expert_cap.shape[0]
    hidden = w_in.shape[2]
    by_patch = jnp.transpose(patches, (1, 0, 2))
    vmem = pl.BlockSpec(memory_space=pltpu.VMEM)
    smem = pl.BlockSpec(memory_space=pltpu.SMEM)
    any_ = pl.BlockSpec(memory_space=pl.ANY)
    blk = (experts, 8, 2 * width + 3 * LANES)
    dma = pltpu.SemaphoreType.DMA
    done = jax.ShapeDtypeStruct((toks, width), BF16)
    result = pl.pallas_call(
        layer_kernel,
        out_shape=done,
        in_specs=[any_, smem] + [vmem] * 5 + [any_, vmem, any_, vmem],
        out_specs=any_,
        scratch_shapes=[
            pltpu.VMEM(by_patch.shape, BF16),
            pltpu.VMEM(blk, BF16),
            pltpu.VMEM(blk, BF16),
            pltpu.VMEM(blk, BF16),
            pltpu.VMEM(blk, BF16),
            pltpu.VMEM((width, hidden), BF16),
            pltpu.VMEM((hidden, width), BF16),
            pltpu.VMEM((SLOTS, width), BF16),
            pltpu.VMEM((SLOTS, hidden), BF16),
            pltpu.VMEM((SLOTS, 1024), F32),
            pltpu.VMEM((SLOTS, 1024), F32),
            pltpu.VMEM((3, 8 * CHUNK, LANES), F32),
            pltpu.VMEM((toks, width), BF16),
            pltpu.VMEM((toks, width), BF16),
            pltpu.VMEM((toks, width), BF16),
            pltpu.VMEM((toks, LANES), F32),
            pltpu.VMEM((CHUNKS, toks, SLOTS), BF16),
            pltpu.VMEM((toks, width), F32),
            dma((3,)),
            dma((experts,)),
            dma((experts,)),
            dma((experts,)),
            dma((experts,)),
        ],
        compiler_params=pltpu.CompilerParams(
            collective_id=0, has_side_effects=True, vmem_limit_bytes=63 * 2**20
        ),
        name="layer",
    )(
        by_patch, visible, routes.reshape(1, toks), expert_cap.reshape(1, experts),
        norm_gain.reshape(1, width), norm_bias.reshape(1, width), router.T, w_in, b_in, w_out, b_out,
    )
    pieces = 7
    return pl.pallas_call(
        finish_kernel,
        out_shape=done,
        in_specs=[any_],
        out_specs=any_,
        scratch_shapes=[pltpu.VMEM((toks, width), BF16), dma((pieces,)), dma((pieces,))],
        name="finish",
    )(result)


def solution(mesh):
    return jax.shard_map(
        per_device,
        mesh=mesh,
        in_specs=(
            P(("dp", "expert"), None, None),
            P(("dp", "expert"), None),
            P(("dp", "expert"), None),
            P("dp"),
            P(),
            P(),
            P(),
            P("expert", None, None),
            P("expert", None),
            P("expert", None, None),
            P("expert", None),
        ),
        out_specs=P(("dp", "expert"), None),
        check_vma=False,
    )
```

```python
import jax
import jax.numpy as jnp
from jax import lax
from jax.experimental import pallas as pl
from jax.experimental.pallas import tpu as pltpu
from jax.sharding import PartitionSpec as P

MESH = pl.DeviceIdType.MESH
SIDE = 4
LANES = 128
PARTNERS = SIDE**3
TURN = 37
BACKTURN = 45
CHUNK = 16
HIGH = 16 * CHUNK
SLOTS = 19 * CHUNK
CHUNKS = PARTNERS // CHUNK
F32 = jnp.float32
BF16 = jnp.bfloat16


def iota(shape, dim):
    return lax.broadcasted_iota(jnp.int32, shape, dim)


def layer_kernel(
    patches, visible_in, route_in, cap_in, gain_in, bias_in, router_in, w_in, b_in_in, w_out, b_out_in,
    out, store_a, store_b, visible, route, cap, gain, bias, router, b_in, b_out, sent, got, made, back, w1, w2,
    rows, act, even, odd, tail, picked, ordered, gate, sel, total,
    load_sem, s_sem, r_sem, ys_sem, yr_sem,
):
    images, width = patches.shape[1], patches.shape[2]
    keep = visible.shape[1]
    toks = images * keep
    experts = cap.shape[1]
    hidden = w1.shape[1]
    me = lax.axis_index("expert")
    mx, my, mz = me // (SIDE * SIDE), (me // SIDE) % SIDE, me % SIDE

    def partner(i, sign):
        code = (i * TURN) % PARTNERS
        x = (mx + sign * (code // (SIDE * SIDE)) + SIDE) % SIDE
        y = (my + sign * ((code // SIDE) % SIDE) + SIDE) % SIDE
        z = (mz + sign * (code % SIDE) + SIDE) % SIDE
        return (x * SIDE + y) * SIDE + z

    small = [
        pltpu.make_async_copy(src, dst, load_sem.at[n])
        for n, (src, dst) in enumerate(
            (
                (route_in, route), (cap_in, cap), (visible_in, visible), (gain_in, gain),
                (bias_in, bias), (router_in, router), (b_in_in, b_in), (b_out_in, b_out),
            )
        )
    ]
    split = width // 2
    load = [
        pltpu.make_async_copy(
            patches.at[:, :, n * split : (n + 1) * split],
            store,
            load_sem.at[len(small) + n],
        )
        for n, store in enumerate((store_a, store_b))
    ]
    for copy in small[:3] + load + small[3:]:
        copy.start()
    barrier = pltpu.get_barrier_semaphore()
    for i in range(1, PARTNERS):
        pl.semaphore_signal(barrier, inc=1, device_id={"expert": partner(i, 1)}, device_id_type=MESH)

    def place(shape, dim):
        t = iota(shape, dim)
        return (t % images) * keep + t // images

    def slot_of(block, rank):
        j = block % CHUNK
        inside = jnp.where(
            rank < 8,
            j * 8 + rank,
            jnp.where(rank < 16, 8 * CHUNK + j * 8 + rank - 8, rank * CHUNK + j),
        )
        return (block // CHUNK) * SLOTS + inside

    def block_of(expert):
        x = (expert // (SIDE * SIDE) - mx + SIDE) % SIDE
        y = ((expert // SIDE) % SIDE - my + SIDE) % SIDE
        z = (expert % SIDE - mz + SIDE) % SIDE
        return (((x * SIDE + y) * SIDE + z) * BACKTURN) % PARTNERS

    small[0].wait()
    small[1].wait()
    diag = iota((experts, experts), 0) == iota((experts, experts), 1)
    cap_col = jnp.sum(jnp.where(diag, cap[...], 0), axis=1, keepdims=True)
    route_b = jnp.broadcast_to(route[...], (8, toks)).astype(F32).astype(BF16)
    to_picked = (iota((toks, 1), 0) == place((1, toks), 1)).astype(BF16)
    route_p = jnp.dot(route_b, to_picked, preferred_element_type=F32)[:1].astype(jnp.int32)
    one_row = iota((experts, toks), 0) == route_p
    ones = one_row.astype(F32)
    earlier = (place((toks, 1), 0) < place((1, toks), 1)).astype(BF16)
    before = jnp.dot(ones.astype(BF16), earlier, preferred_element_type=F32)
    rank = jnp.sum(before * ones, axis=0, keepdims=True).astype(jnp.int32)
    limit = jnp.sum(jnp.where(one_row, cap_col, 0), axis=0, keepdims=True)
    key = jnp.where(rank < limit, slot_of(block_of(route_p), rank), -1)

    small[2].wait()
    row = iota((images, split), 0)
    for n, store in enumerate((store_a, store_b)):
        load[n].wait()

        def pick(k, carry, store=store, lanes=slice(n * split, (n + 1) * split)):
            val = store[visible[0, k]]
            for i in range(1, images):
                val = jnp.where(row == i, store[visible[i, k]], val)
            picked[pl.ds(pl.multiple_of(k * images, images), images), lanes] = val
            return carry

        lax.fori_loop(0, keep, pick, 0, unroll=7)

    load1 = pltpu.make_async_copy(w_in.at[0], w1, load_sem.at[10])
    load1.start()
    load2 = pltpu.make_async_copy(w_out.at[0], w2, load_sem.at[11])
    load2.start()

    def normed(xf):
        mean = jnp.sum(xf, axis=1, keepdims=True) * (1.0 / width)
        diff = xf - mean
        var = jnp.sum(diff * diff, axis=1, keepdims=True) * (1.0 / width)
        return diff * (1.0 / jnp.sqrt(var + 1e-06)) * gain[...] + bias[...]

    def out_copy(i):
        return pltpu.make_async_remote_copy(
            src_ref=sent.at[i], dst_ref=got.at[i], send_sem=s_sem.at[i], recv_sem=r_sem.at[i],
            device_id={"expert": partner(i, 1)}, device_id_type=MESH,
        )

    def back_copy(i):
        return pltpu.make_async_remote_copy(
            src_ref=made.at[i], dst_ref=back.at[i], send_sem=ys_sem.at[i], recv_sem=yr_sem.at[i],
            device_id={"expert": partner(i, -1)}, device_id_type=MESH,
        )

    half = 8 * CHUNK

    def each(c, act_on):
        @pl.when(c > 0)
        def _():
            act_on(c * CHUNK)

        for i in range(1, CHUNK):
            act_on(c * CHUNK + i)

    def put(ref, lo, y):
        span = pl.ds(lo, CHUNK)
        for part in range(2):
            ref[span, :, part * width : (part + 1) * width] = (
                y[part * half : (part + 1) * half].reshape(CHUNK, 8, width).astype(BF16)
            )
        for r in range(3):
            first = HIGH + r * CHUNK
            for j in range(8):
                tail[r, pl.ds(j, CHUNK, stride=8), :] = y[
                    first : first + CHUNK, j * LANES : (j + 1) * LANES
                ]
            lanes = slice(2 * width + r * LANES, 2 * width + (r + 1) * LANES)
            ref[span, :, lanes] = tail[r].reshape(CHUNK, 8, LANES).astype(BF16)

    def take(ref, lo):
        span = pl.ds(lo, CHUNK)
        for part in range(2):
            piece = ref[span, :, part * width : (part + 1) * width]
            rows[part * half : (part + 1) * half, :] = (
                piece.astype(F32).reshape(half, width).astype(BF16)
            )
        for r in range(3):
            lanes = slice(2 * width + r * LANES, 2 * width + (r + 1) * LANES)
            tail[r] = ref[span, :, lanes].astype(F32).reshape(half, LANES)
            for j in range(8):
                first = HIGH + r * CHUNK
                rows[first : first + CHUNK, j * LANES : (j + 1) * LANES] = tail[
                    r, pl.ds(j, CHUNK, stride=8), :
                ].astype(BF16)

    @pl.loop(0, CHUNKS)
    def _(c):
        chosen = (iota((SLOTS, toks), 0) + c * SLOTS == key).astype(BF16)
        put(sent, c * CHUNK, jnp.dot(chosen, picked[...], preferred_element_type=F32))

        @pl.when(c == 0)
        def _():
            pl.semaphore_wait(barrier, PARTNERS - 1)
            got[0] = sent[0]

        each(c, lambda i: out_copy(i).start())

    for copy in small[3:]:
        copy.wait()

    total[...] = jnp.zeros_like(total)
    to_own = (place((1, toks), 1) == iota((toks, 1), 0)).astype(BF16)
    ordered[...] = jnp.dot(to_own, picked[...], preferred_element_type=F32).astype(BF16)
    eye = (iota((toks, 1), 0) == iota((1, toks), 1)).astype(BF16)

    def product(a, b):
        return lax.dot_general(a, b, (((1,), (1,)), ((), ())), preferred_element_type=F32)

    route_c = product(eye, route_b)[:, :1].astype(jnp.int32)
    one_col = iota((toks, experts), 1) == route_c
    ones_c = one_col.astype(F32)
    lower = (iota((toks, 1), 0) > iota((1, toks), 1)).astype(BF16)
    before_c = jnp.dot(lower, ones_c.astype(BF16), preferred_element_type=F32)
    rank_c = jnp.sum(before_c * ones_c, axis=1, keepdims=True).astype(jnp.int32)
    limit_c = jnp.sum(jnp.where(one_col, cap[...], 0), axis=1, keepdims=True)
    block_c = jnp.sum(
        jnp.where(one_col, block_of(iota((1, experts), 1)), 0), axis=1, keepdims=True
    )
    key_c = jnp.where(rank_c < limit_c, slot_of(block_c, rank_c), -1)
    for c in range(CHUNKS):
        sel[c] = (iota((toks, SLOTS), 1) + c * SLOTS == key_c).astype(BF16)

    r_full = router[...]
    r_hi = r_full.astype(BF16)
    r_lo = (r_full - r_hi.astype(F32)).astype(BF16)
    group = 7 * images
    for g in range(toks // group):
        span = slice(g * group, (g + 1) * group)
        h = normed(ordered[span, :].astype(F32))
        h_hi = h.astype(BF16)
        h_lo = (h - h_hi.astype(F32)).astype(BF16)
        logits = product(h_hi, r_lo) + product(h_lo, r_hi) + product(h_hi, r_hi)
        score = jnp.sum(logits * ones_c[span], axis=1, keepdims=True)
        gate[span, :] = jnp.broadcast_to(1.0 / (1.0 + jnp.exp(-score)), (group, LANES))

    step = 1024
    last = hidden - step

    def enter(f, ref):
        ref[...] = jnp.dot(rows[...], w1[:, f : f + step], preferred_element_type=F32)

    def bend(f, ref):
        v = ref[...] + b_in[:, f : f + step]
        inner = v * (0.7978845608028654 + 0.035677408136300125 * (v * v))
        half_v = 0.5 * v
        act[:, f : f + step] = (half_v + half_v * jnp.tanh(inner)).astype(BF16)

    load1.wait()
    load2.wait()

    @pl.loop(0, CHUNKS)
    def _(c):
        each(c, lambda i: out_copy(i).wait_recv())
        take(got, c * CHUNK)
        for g in range(SLOTS // CHUNK):
            span = slice(g * CHUNK, (g + 1) * CHUNK)
            rows[span, :] = normed(rows[span, :].astype(F32)).astype(BF16)
        spare = (even, odd)
        enter(0, even)
        for n in range(1, hidden // step):
            enter(n * step, spare[n % 2])
            bend((n - 1) * step, spare[(n - 1) % 2])
        y = jnp.dot(act[:, :last], w2[:last, :], preferred_element_type=F32)
        bend(last, spare[(hidden // step - 1) % 2])
        y = y + jnp.dot(act[:, last:], w2[last:, :], preferred_element_type=F32)
        put(made, c * CHUNK, y + b_out[...])
        each(c, lambda i: back_copy(i).start())

        @pl.when(c == 0)
        def _():
            back[0] = made[0]

        @pl.when(c >= 2)
        def _():
            each(c - 2, lambda i: back_copy(i).wait_recv())
            take(back, (c - 2) * CHUNK)
            total[...] += jnp.dot(sel[c - 2], rows[...], preferred_element_type=F32)

    @pl.loop(1, PARTNERS)
    def _(i):
        out_copy(i).wait_send()

    c = CHUNKS - 2
    each(c, lambda i: back_copy(i).wait_recv())
    take(back, c * CHUNK)
    total[...] += jnp.dot(sel[c], rows[...], preferred_element_type=F32)
    c = CHUNKS - 1
    each(c, lambda i: back_copy(i).wait_recv())
    take(back, c * CHUNK)
    wide = width // 2
    for n in range(2):
        cols = slice(n * wide, (n + 1) * wide)
        part = total[:, cols] + jnp.dot(sel[c], rows[:, cols], preferred_element_type=F32)
        out[:, cols] = (ordered[:, cols].astype(F32) + gate[:, :1] * part).astype(BF16)

    @pl.loop(1, PARTNERS)
    def _(i):
        back_copy(i).wait_send()


def finish_kernel(src, out, sem):
    size = src.shape[0] // sem.shape[0]
    stores = [
        pltpu.make_async_copy(src.at[pl.ds(n * size, size)], out.at[pl.ds(n * size, size)], sem.at[n])
        for n in range(sem.shape[0])
    ]
    for copy in stores:
        copy.start()
    for copy in stores:
        copy.wait()


def per_device(
    patches, visible, routes, expert_cap, norm_gain, norm_bias, router, w_in, b_in, w_out, b_out
):
    images, _, width = patches.shape
    toks = images * visible.shape[1]
    experts = expert_cap.shape[0]
    hidden = w_in.shape[2]
    by_patch = jnp.transpose(patches, (1, 0, 2))
    vmem = pl.BlockSpec(memory_space=pltpu.VMEM)
    any_ = pl.BlockSpec(memory_space=pl.ANY)
    blk = (experts, 8, 2 * width + 3 * LANES)
    dma = pltpu.SemaphoreType.DMA
    done = jax.ShapeDtypeStruct((toks, width), BF16)
    result = pl.pallas_call(
        layer_kernel,
        out_shape=pltpu.VMEM((toks, width), BF16),
        in_specs=[any_] * 11,
        out_specs=vmem,
        scratch_shapes=[
            pltpu.VMEM(by_patch.shape[:2] + (width // 2,), BF16),
            pltpu.VMEM(by_patch.shape[:2] + (width // 2,), BF16),
            pltpu.SMEM(visible.shape, jnp.int32),
            pltpu.VMEM((1, toks), jnp.int32),
            pltpu.VMEM((1, experts), jnp.int32),
            pltpu.VMEM((1, width), F32),
            pltpu.VMEM((1, width), F32),
            pltpu.VMEM((experts, width), F32),
            pltpu.VMEM((1, hidden), F32),
            pltpu.VMEM((1, width), F32),
            pltpu.VMEM(blk, BF16),
            pltpu.VMEM(blk, BF16),
            pltpu.VMEM(blk, BF16),
            pltpu.VMEM(blk, BF16),
            pltpu.VMEM((width, hidden), BF16),
            pltpu.VMEM((hidden, width), BF16),
            pltpu.VMEM((SLOTS, width), BF16),
            pltpu.VMEM((SLOTS, hidden), BF16),
            pltpu.VMEM((SLOTS, 1024), F32),
            pltpu.VMEM((SLOTS, 1024), F32),
            pltpu.VMEM((3, 8 * CHUNK, LANES), F32),
            pltpu.VMEM((toks, width), BF16),
            pltpu.VMEM((toks, width), BF16),
            pltpu.VMEM((toks, LANES), F32),
            pltpu.VMEM((CHUNKS, toks, SLOTS), BF16),
            pltpu.VMEM((toks, width), F32),
            dma((12,)),
            dma((experts,)),
            dma((experts,)),
            dma((experts,)),
            dma((experts,)),
        ],
        compiler_params=pltpu.CompilerParams(
            collective_id=0, has_side_effects=True, vmem_limit_bytes=58 * 2**20
        ),
        name="layer",
    )(
        by_patch, visible, routes.reshape(1, toks), expert_cap.reshape(1, experts),
        norm_gain.reshape(1, width), norm_bias.reshape(1, width), router.T, w_in, b_in, w_out, b_out,
    )
    pieces = 2
    return pl.pallas_call(
        finish_kernel,
        out_shape=done,
        in_specs=[vmem],
        out_specs=any_,
        scratch_shapes=[dma((pieces,))],
        compiler_params=pltpu.CompilerParams(vmem_limit_bytes=4 * 2**20),
        name="finish",
    )(result)


def solution(mesh):
    return jax.shard_map(
        per_device,
        mesh=mesh,
        in_specs=(
            P(("dp", "expert"), None, None),
            P(("dp", "expert"), None),
            P(("dp", "expert"), None),
            P("dp"),
            P(),
            P(),
            P(),
            P("expert", None, None),
            P("expert", None),
            P("expert", None, None),
            P("expert", None),
        ),
        out_specs=P(("dp", "expert"), None),
        check_vma=False,
    )
```

```python
import jax
import jax.numpy as jnp
from jax import lax
from jax.experimental import pallas as pl
from jax.experimental.pallas import tpu as pltpu
from jax.sharding import PartitionSpec as P

MESH = pl.DeviceIdType.MESH
SIDE = 4
LANES = 128
PARTNERS = SIDE**3
TURN = 25
BACKTURN = 41
CHUNK = 16
HIGH = 16 * CHUNK
SLOTS = 19 * CHUNK
CHUNKS = PARTNERS // CHUNK
F32 = jnp.float32
BF16 = jnp.bfloat16


def iota(shape, dim):
    return lax.broadcasted_iota(jnp.int32, shape, dim)


def layer_kernel(
    patches, visible_in, route_in, cap_in, gain_in, bias_in, router_in, w_in, b_in_in, w_out, b_out_in,
    out, store_a, store_b, visible, route, cap, gain, bias, router, b_in, b_out, sent, got, made, back, w1, w2,
    rows, act, even, odd, tail, picked, ordered, gate, sel, total,
    load_sem, s_sem, r_sem, ys_sem, yr_sem,
):
    images, width = patches.shape[1], patches.shape[2]
    keep = visible.shape[1]
    toks = images * keep
    experts = cap.shape[1]
    hidden = w1.shape[1]
    me = lax.axis_index("expert")
    mx, my, mz = me // (SIDE * SIDE), (me // SIDE) % SIDE, me % SIDE

    def partner(i, sign):
        code = (i * TURN) % PARTNERS
        x = (mx + sign * (code // (SIDE * SIDE)) + SIDE) % SIDE
        y = (my + sign * ((code // SIDE) % SIDE) + SIDE) % SIDE
        z = (mz + sign * (code % SIDE) + SIDE) % SIDE
        return (x * SIDE + y) * SIDE + z

    small = [
        pltpu.make_async_copy(src, dst, load_sem.at[n])
        for n, (src, dst) in enumerate(
            (
                (route_in, route), (cap_in, cap), (visible_in, visible), (gain_in, gain),
                (bias_in, bias), (router_in, router), (b_in_in, b_in), (b_out_in, b_out),
            )
        )
    ]
    split = width // 2
    load = [
        pltpu.make_async_copy(
            patches.at[:, :, n * split : (n + 1) * split],
            store,
            load_sem.at[len(small) + n],
        )
        for n, store in enumerate((store_a, store_b))
    ]
    for copy in small[:3] + load + small[3:]:
        copy.start()
    barrier = pltpu.get_barrier_semaphore()
    for i in range(1, PARTNERS):
        pl.semaphore_signal(barrier, inc=1, device_id={"expert": partner(i, 1)}, device_id_type=MESH)

    def place(shape, dim):
        t = iota(shape, dim)
        return (t % images) * keep + t // images

    def slot_of(block, rank):
        j = block % CHUNK
        inside = jnp.where(
            rank < 8,
            j * 8 + rank,
            jnp.where(rank < 16, 8 * CHUNK + j * 8 + rank - 8, rank * CHUNK + j),
        )
        return (block // CHUNK) * SLOTS + inside

    def block_of(expert):
        x = (expert // (SIDE * SIDE) - mx + SIDE) % SIDE
        y = ((expert // SIDE) % SIDE - my + SIDE) % SIDE
        z = (expert % SIDE - mz + SIDE) % SIDE
        return (((x * SIDE + y) * SIDE + z) * BACKTURN) % PARTNERS

    small[0].wait()
    small[1].wait()
    diag = iota((experts, experts), 0) == iota((experts, experts), 1)
    cap_col = jnp.sum(jnp.where(diag, cap[...], 0), axis=1, keepdims=True)
    route_b = jnp.broadcast_to(route[...], (8, toks)).astype(F32).astype(BF16)
    to_picked = (iota((toks, 1), 0) == place((1, toks), 1)).astype(BF16)
    route_p = jnp.dot(route_b, to_picked, preferred_element_type=F32)[:1].astype(jnp.int32)
    one_row = iota((experts, toks), 0) == route_p
    ones = one_row.astype(F32)
    earlier = (place((toks, 1), 0) < place((1, toks), 1)).astype(BF16)
    before = jnp.dot(ones.astype(BF16), earlier, preferred_element_type=F32)
    rank = jnp.sum(before * ones, axis=0, keepdims=True).astype(jnp.int32)
    limit = jnp.sum(jnp.where(one_row, cap_col, 0), axis=0, keepdims=True)
    key = jnp.where(rank < limit, slot_of(block_of(route_p), rank), -1)

    small[2].wait()
    row = iota((images, split), 0)
    for n, store in enumerate((store_a, store_b)):
        load[n].wait()

        def pick(k, carry, store=store, lanes=slice(n * split, (n + 1) * split)):
            val = store[visible[0, k]]
            for i in range(1, images):
                val = jnp.where(row == i, store[visible[i, k]], val)
            picked[pl.ds(pl.multiple_of(k * images, images), images), lanes] = val
            return carry

        lax.fori_loop(0, keep, pick, 0, unroll=7)

    load1 = pltpu.make_async_copy(w_in.at[0], w1, load_sem.at[10])
    load1.start()
    load2 = pltpu.make_async_copy(w_out.at[0], w2, load_sem.at[11])
    load2.start()

    def normed(xf):
        mean = jnp.sum(xf, axis=1, keepdims=True) * (1.0 / width)
        diff = xf - mean
        var = jnp.sum(diff * diff, axis=1, keepdims=True) * (1.0 / width)
        return diff * (1.0 / jnp.sqrt(var + 1e-06)) * gain[...] + bias[...]

    def out_copy(i):
        return pltpu.make_async_remote_copy(
            src_ref=sent.at[i], dst_ref=got.at[i], send_sem=s_sem.at[i], recv_sem=r_sem.at[i],
            device_id={"expert": partner(i, 1)}, device_id_type=MESH,
        )

    def back_copy(i):
        return pltpu.make_async_remote_copy(
            src_ref=made.at[i], dst_ref=back.at[i], send_sem=ys_sem.at[i], recv_sem=yr_sem.at[i],
            device_id={"expert": partner(i, -1)}, device_id_type=MESH,
        )

    half = 8 * CHUNK

    def each(c, act_on):
        @pl.when(c > 0)
        def _():
            act_on(c * CHUNK)

        for i in range(1, CHUNK):
            act_on(c * CHUNK + i)

    def put(ref, lo, y):
        span = pl.ds(lo, CHUNK)
        for part in range(2):
            ref[span, :, part * width : (part + 1) * width] = (
                y[part * half : (part + 1) * half].reshape(CHUNK, 8, width).astype(BF16)
            )
        for r in range(3):
            first = HIGH + r * CHUNK
            for j in range(8):
                tail[r, pl.ds(j, CHUNK, stride=8), :] = y[
                    first : first + CHUNK, j * LANES : (j + 1) * LANES
                ]
            lanes = slice(2 * width + r * LANES, 2 * width + (r + 1) * LANES)
            ref[span, :, lanes] = tail[r].reshape(CHUNK, 8, LANES).astype(BF16)

    def take(ref, lo):
        span = pl.ds(lo, CHUNK)
        for part in range(2):
            piece = ref[span, :, part * width : (part + 1) * width]
            rows[part * half : (part + 1) * half, :] = (
                piece.astype(F32).reshape(half, width).astype(BF16)
            )
        for r in range(3):
            lanes = slice(2 * width + r * LANES, 2 * width + (r + 1) * LANES)
            tail[r] = ref[span, :, lanes].astype(F32).reshape(half, LANES)
            for j in range(8):
                first = HIGH + r * CHUNK
                rows[first : first + CHUNK, j * LANES : (j + 1) * LANES] = tail[
                    r, pl.ds(j, CHUNK, stride=8), :
                ].astype(BF16)

    @pl.loop(0, CHUNKS)
    def _(c):
        chosen = (iota((SLOTS, toks), 0) + c * SLOTS == key).astype(BF16)
        put(sent, c * CHUNK, jnp.dot(chosen, picked[...], preferred_element_type=F32))

        @pl.when(c == 0)
        def _():
            pl.semaphore_wait(barrier, PARTNERS - 1)
            got[0] = sent[0]

        each(c, lambda i: out_copy(i).start())

    for copy in small[3:]:
        copy.wait()

    total[...] = jnp.zeros_like(total)
    to_own = (place((1, toks), 1) == iota((toks, 1), 0)).astype(BF16)
    ordered[...] = jnp.dot(to_own, picked[...], preferred_element_type=F32).astype(BF16)
    eye = (iota((toks, 1), 0) == iota((1, toks), 1)).astype(BF16)

    def product(a, b):
        return lax.dot_general(a, b, (((1,), (1,)), ((), ())), preferred_element_type=F32)

    route_c = product(eye, route_b)[:, :1].astype(jnp.int32)
    one_col = iota((toks, experts), 1) == route_c
    ones_c = one_col.astype(F32)
    lower = (iota((toks, 1), 0) > iota((1, toks), 1)).astype(BF16)
    before_c = jnp.dot(lower, ones_c.astype(BF16), preferred_element_type=F32)
    rank_c = jnp.sum(before_c * ones_c, axis=1, keepdims=True).astype(jnp.int32)
    limit_c = jnp.sum(jnp.where(one_col, cap[...], 0), axis=1, keepdims=True)
    block_c = jnp.sum(
        jnp.where(one_col, block_of(iota((1, experts), 1)), 0), axis=1, keepdims=True
    )
    key_c = jnp.where(rank_c < limit_c, slot_of(block_c, rank_c), -1)
    for c in range(CHUNKS):
        sel[c] = (iota((toks, SLOTS), 1) + c * SLOTS == key_c).astype(BF16)

    r_full = router[...]
    r_hi = r_full.astype(BF16)
    r_lo = (r_full - r_hi.astype(F32)).astype(BF16)
    group = 7 * images
    for g in range(toks // group):
        span = slice(g * group, (g + 1) * group)
        h = normed(ordered[span, :].astype(F32))
        h_hi = h.astype(BF16)
        h_lo = (h - h_hi.astype(F32)).astype(BF16)
        logits = product(h_hi, r_lo) + product(h_lo, r_hi) + product(h_hi, r_hi)
        score = jnp.sum(logits * ones_c[span], axis=1, keepdims=True)
        gate[span, :] = jnp.broadcast_to(1.0 / (1.0 + jnp.exp(-score)), (group, LANES))

    step = 1024
    last = hidden - step

    def enter(f, ref):
        ref[...] = jnp.dot(rows[...], w1[:, f : f + step], preferred_element_type=F32)

    def bend(f, ref):
        v = ref[...] + b_in[:, f : f + step]
        inner = v * (0.7978845608028654 + 0.035677408136300125 * (v * v))
        half_v = 0.5 * v
        act[:, f : f + step] = (half_v + half_v * jnp.tanh(inner)).astype(BF16)

    load1.wait()
    load2.wait()

    @pl.loop(0, CHUNKS)
    def _(c):
        each(c, lambda i: out_copy(i).wait_recv())
        take(got, c * CHUNK)
        for g in range(SLOTS // CHUNK):
            span = slice(g * CHUNK, (g + 1) * CHUNK)
            rows[span, :] = normed(rows[span, :].astype(F32)).astype(BF16)
        spare = (even, odd)
        enter(0, even)
        for n in range(1, hidden // step):
            enter(n * step, spare[n % 2])
            bend((n - 1) * step, spare[(n - 1) % 2])
        y = jnp.dot(act[:, :last], w2[:last, :], preferred_element_type=F32)
        bend(last, spare[(hidden // step - 1) % 2])
        y = y + jnp.dot(act[:, last:], w2[last:, :], preferred_element_type=F32)
        put(made, c * CHUNK, y + b_out[...])
        each(c, lambda i: back_copy(i).start())

        @pl.when(c == 0)
        def _():
            back[0] = made[0]

        @pl.when(c >= 2)
        def _():
            each(c - 2, lambda i: back_copy(i).wait_recv())
            take(back, (c - 2) * CHUNK)
            total[...] += jnp.dot(sel[c - 2], rows[...], preferred_element_type=F32)

    @pl.loop(1, PARTNERS)
    def _(i):
        out_copy(i).wait_send()

    c = CHUNKS - 2
    each(c, lambda i: back_copy(i).wait_recv())
    take(back, c * CHUNK)
    total[...] += jnp.dot(sel[c], rows[...], preferred_element_type=F32)
    c = CHUNKS - 1
    each(c, lambda i: back_copy(i).wait_recv())
    take(back, c * CHUNK)
    wide = width // 2
    for n in range(2):
        cols = slice(n * wide, (n + 1) * wide)
        part = total[:, cols] + jnp.dot(sel[c], rows[:, cols], preferred_element_type=F32)
        out[:, cols] = (ordered[:, cols].astype(F32) + gate[:, :1] * part).astype(BF16)

    @pl.loop(1, PARTNERS)
    def _(i):
        back_copy(i).wait_send()


def finish_kernel(src, out, sem):
    size = src.shape[0] // sem.shape[0]
    stores = [
        pltpu.make_async_copy(src.at[pl.ds(n * size, size)], out.at[pl.ds(n * size, size)], sem.at[n])
        for n in range(sem.shape[0])
    ]
    for copy in stores:
        copy.start()
    for copy in stores:
        copy.wait()


def per_device(
    patches, visible, routes, expert_cap, norm_gain, norm_bias, router, w_in, b_in, w_out, b_out
):
    images, _, width = patches.shape
    toks = images * visible.shape[1]
    experts = expert_cap.shape[0]
    hidden = w_in.shape[2]
    by_patch = jnp.transpose(patches, (1, 0, 2))
    vmem = pl.BlockSpec(memory_space=pltpu.VMEM)
    any_ = pl.BlockSpec(memory_space=pl.ANY)
    blk = (experts, 8, 2 * width + 3 * LANES)
    dma = pltpu.SemaphoreType.DMA
    done = jax.ShapeDtypeStruct((toks, width), BF16)
    result = pl.pallas_call(
        layer_kernel,
        out_shape=pltpu.VMEM((toks, width), BF16),
        in_specs=[any_] * 11,
        out_specs=vmem,
        scratch_shapes=[
            pltpu.VMEM(by_patch.shape[:2] + (width // 2,), BF16),
            pltpu.VMEM(by_patch.shape[:2] + (width // 2,), BF16),
            pltpu.SMEM(visible.shape, jnp.int32),
            pltpu.VMEM((1, toks), jnp.int32),
            pltpu.VMEM((1, experts), jnp.int32),
            pltpu.VMEM((1, width), F32),
            pltpu.VMEM((1, width), F32),
            pltpu.VMEM((experts, width), F32),
            pltpu.VMEM((1, hidden), F32),
            pltpu.VMEM((1, width), F32),
            pltpu.VMEM(blk, BF16),
            pltpu.VMEM(blk, BF16),
            pltpu.VMEM(blk, BF16),
            pltpu.VMEM(blk, BF16),
            pltpu.VMEM((width, hidden), BF16),
            pltpu.VMEM((hidden, width), BF16),
            pltpu.VMEM((SLOTS, width), BF16),
            pltpu.VMEM((SLOTS, hidden), BF16),
            pltpu.VMEM((SLOTS, 1024), F32),
            pltpu.VMEM((SLOTS, 1024), F32),
            pltpu.VMEM((3, 8 * CHUNK, LANES), F32),
            pltpu.VMEM((toks, width), BF16),
            pltpu.VMEM((toks, width), BF16),
            pltpu.VMEM((toks, LANES), F32),
            pltpu.VMEM((CHUNKS, toks, SLOTS), BF16),
            pltpu.VMEM((toks, width), F32),
            dma((12,)),
            dma((experts,)),
            dma((experts,)),
            dma((experts,)),
            dma((experts,)),
        ],
        compiler_params=pltpu.CompilerParams(
            collective_id=0, has_side_effects=True, vmem_limit_bytes=58 * 2**20
        ),
        name="layer",
    )(
        by_patch, visible, routes.reshape(1, toks), expert_cap.reshape(1, experts),
        norm_gain.reshape(1, width), norm_bias.reshape(1, width), router.T, w_in, b_in, w_out, b_out,
    )
    pieces = 2
    return pl.pallas_call(
        finish_kernel,
        out_shape=done,
        in_specs=[vmem],
        out_specs=any_,
        scratch_shapes=[dma((pieces,))],
        compiler_params=pltpu.CompilerParams(vmem_limit_bytes=4 * 2**20),
        name="finish",
    )(result)


def solution(mesh):
    return jax.shard_map(
        per_device,
        mesh=mesh,
        in_specs=(
            P(("dp", "expert"), None, None),
            P(("dp", "expert"), None),
            P(("dp", "expert"), None),
            P("dp"),
            P(),
            P(),
            P(),
            P("expert", None, None),
            P("expert", None),
            P("expert", None, None),
            P("expert", None),
        ),
        out_specs=P(("dp", "expert"), None),
        check_vma=False,
    )
```

```python
import jax
import jax.numpy as jnp
from jax import lax
from jax.experimental import pallas as pl
from jax.experimental.pallas import tpu as pltpu
from jax.sharding import PartitionSpec as P

MESH = pl.DeviceIdType.MESH
SIDE = 4
LANES = 128
PARTNERS = SIDE**3
TURN = 41
BACKTURN = 25
CHUNK = 16
HIGH = 16 * CHUNK
SLOTS = 19 * CHUNK
CHUNKS = PARTNERS // CHUNK
F32 = jnp.float32
BF16 = jnp.bfloat16


def iota(shape, dim):
    return lax.broadcasted_iota(jnp.int32, shape, dim)


def layer_kernel(
    patches, visible_in, route_in, cap_in, gain_in, bias_in, router_in, w_in, b_in_in, w_out, b_out_in,
    out, store_a, store_b, visible, route, cap, gain, bias, router, b_in, b_out, sent, got, made, back, w1, w2,
    rows, act, even, odd, tail, picked, ordered, gate, sel, total,
    load_sem, s_sem, r_sem, ys_sem, yr_sem,
):
    images, width = patches.shape[1], patches.shape[2]
    keep = visible.shape[1]
    toks = images * keep
    experts = cap.shape[1]
    hidden = w1.shape[1]
    me = lax.axis_index("expert")
    mx, my, mz = me // (SIDE * SIDE), (me // SIDE) % SIDE, me % SIDE

    def partner(i, sign):
        code = (i * TURN) % PARTNERS
        x = (mx + sign * (code // (SIDE * SIDE)) + SIDE) % SIDE
        y = (my + sign * ((code // SIDE) % SIDE) + SIDE) % SIDE
        z = (mz + sign * (code % SIDE) + SIDE) % SIDE
        return (x * SIDE + y) * SIDE + z

    small = [
        pltpu.make_async_copy(src, dst, load_sem.at[n])
        for n, (src, dst) in enumerate(
            (
                (route_in, route), (cap_in, cap), (visible_in, visible), (gain_in, gain),
                (bias_in, bias), (router_in, router), (b_in_in, b_in), (b_out_in, b_out),
            )
        )
    ]
    split = width // 2
    load = [
        pltpu.make_async_copy(
            patches.at[:, :, n * split : (n + 1) * split],
            store,
            load_sem.at[len(small) + n],
        )
        for n, store in enumerate((store_a, store_b))
    ]
    for copy in small[:3] + load + small[3:]:
        copy.start()
    barrier = pltpu.get_barrier_semaphore()
    for i in range(1, PARTNERS):
        pl.semaphore_signal(barrier, inc=1, device_id={"expert": partner(i, 1)}, device_id_type=MESH)

    def place(shape, dim):
        t = iota(shape, dim)
        return (t % images) * keep + t // images

    def slot_of(block, rank):
        j = block % CHUNK
        inside = jnp.where(
            rank < 8,
            j * 8 + rank,
            jnp.where(rank < 16, 8 * CHUNK + j * 8 + rank - 8, rank * CHUNK + j),
        )
        return (block // CHUNK) * SLOTS + inside

    def block_of(expert):
        x = (expert // (SIDE * SIDE) - mx + SIDE) % SIDE
        y = ((expert // SIDE) % SIDE - my + SIDE) % SIDE
        z = (expert % SIDE - mz + SIDE) % SIDE
        return (((x * SIDE + y) * SIDE + z) * BACKTURN) % PARTNERS

    small[0].wait()
    small[1].wait()
    diag = iota((experts, experts), 0) == iota((experts, experts), 1)
    cap_col = jnp.sum(jnp.where(diag, cap[...], 0), axis=1, keepdims=True)
    route_b = jnp.broadcast_to(route[...], (8, toks)).astype(F32).astype(BF16)
    to_picked = (iota((toks, 1), 0) == place((1, toks), 1)).astype(BF16)
    route_p = jnp.dot(route_b, to_picked, preferred_element_type=F32)[:1].astype(jnp.int32)
    one_row = iota((experts, toks), 0) == route_p
    ones = one_row.astype(F32)
    earlier = (place((toks, 1), 0) < place((1, toks), 1)).astype(BF16)
    before = jnp.dot(ones.astype(BF16), earlier, preferred_element_type=F32)
    rank = jnp.sum(before * ones, axis=0, keepdims=True).astype(jnp.int32)
    limit = jnp.sum(jnp.where(one_row, cap_col, 0), axis=0, keepdims=True)
    key = jnp.where(rank < limit, slot_of(block_of(route_p), rank), -1)

    small[2].wait()
    row = iota((images, split), 0)
    for n, store in enumerate((store_a, store_b)):
        load[n].wait()

        def pick(k, carry, store=store, lanes=slice(n * split, (n + 1) * split)):
            val = store[visible[0, k]]
            for i in range(1, images):
                val = jnp.where(row == i, store[visible[i, k]], val)
            picked[pl.ds(pl.multiple_of(k * images, images), images), lanes] = val
            return carry

        lax.fori_loop(0, keep, pick, 0, unroll=7)

    load1 = pltpu.make_async_copy(w_in.at[0], w1, load_sem.at[10])
    load1.start()
    load2 = pltpu.make_async_copy(w_out.at[0], w2, load_sem.at[11])
    load2.start()

    def normed(xf):
        mean = jnp.sum(xf, axis=1, keepdims=True) * (1.0 / width)
        diff = xf - mean
        var = jnp.sum(diff * diff, axis=1, keepdims=True) * (1.0 / width)
        return diff * (1.0 / jnp.sqrt(var + 1e-06)) * gain[...] + bias[...]

    def out_copy(i):
        return pltpu.make_async_remote_copy(
            src_ref=sent.at[i], dst_ref=got.at[i], send_sem=s_sem.at[i], recv_sem=r_sem.at[i],
            device_id={"expert": partner(i, 1)}, device_id_type=MESH,
        )

    def back_copy(i):
        return pltpu.make_async_remote_copy(
            src_ref=made.at[i], dst_ref=back.at[i], send_sem=ys_sem.at[i], recv_sem=yr_sem.at[i],
            device_id={"expert": partner(i, -1)}, device_id_type=MESH,
        )

    half = 8 * CHUNK

    def each(c, act_on):
        @pl.when(c > 0)
        def _():
            act_on(c * CHUNK)

        for i in range(1, CHUNK):
            act_on(c * CHUNK + i)

    def put(ref, lo, y):
        span = pl.ds(lo, CHUNK)
        for part in range(2):
            ref[span, :, part * width : (part + 1) * width] = (
                y[part * half : (part + 1) * half].reshape(CHUNK, 8, width).astype(BF16)
            )
        for r in range(3):
            first = HIGH + r * CHUNK
            for j in range(8):
                tail[r, pl.ds(j, CHUNK, stride=8), :] = y[
                    first : first + CHUNK, j * LANES : (j + 1) * LANES
                ]
            lanes = slice(2 * width + r * LANES, 2 * width + (r + 1) * LANES)
            ref[span, :, lanes] = tail[r].reshape(CHUNK, 8, LANES).astype(BF16)

    def take(ref, lo):
        span = pl.ds(lo, CHUNK)
        for part in range(2):
            piece = ref[span, :, part * width : (part + 1) * width]
            rows[part * half : (part + 1) * half, :] = (
                piece.astype(F32).reshape(half, width).astype(BF16)
            )
        for r in range(3):
            lanes = slice(2 * width + r * LANES, 2 * width + (r + 1) * LANES)
            tail[r] = ref[span, :, lanes].astype(F32).reshape(half, LANES)
            for j in range(8):
                first = HIGH + r * CHUNK
                rows[first : first + CHUNK, j * LANES : (j + 1) * LANES] = tail[
                    r, pl.ds(j, CHUNK, stride=8), :
                ].astype(BF16)

    @pl.loop(0, CHUNKS)
    def _(c):
        chosen = (iota((SLOTS, toks), 0) + c * SLOTS == key).astype(BF16)
        put(sent, c * CHUNK, jnp.dot(chosen, picked[...], preferred_element_type=F32))

        @pl.when(c == 0)
        def _():
            pl.semaphore_wait(barrier, PARTNERS - 1)
            got[0] = sent[0]

        each(c, lambda i: out_copy(i).start())

    for copy in small[3:]:
        copy.wait()

    total[...] = jnp.zeros_like(total)
    to_own = (place((1, toks), 1) == iota((toks, 1), 0)).astype(BF16)
    ordered[...] = jnp.dot(to_own, picked[...], preferred_element_type=F32).astype(BF16)
    eye = (iota((toks, 1), 0) == iota((1, toks), 1)).astype(BF16)

    def product(a, b):
        return lax.dot_general(a, b, (((1,), (1,)), ((), ())), preferred_element_type=F32)

    route_c = product(eye, route_b)[:, :1].astype(jnp.int32)
    one_col = iota((toks, experts), 1) == route_c
    ones_c = one_col.astype(F32)
    lower = (iota((toks, 1), 0) > iota((1, toks), 1)).astype(BF16)
    before_c = jnp.dot(lower, ones_c.astype(BF16), preferred_element_type=F32)
    rank_c = jnp.sum(before_c * ones_c, axis=1, keepdims=True).astype(jnp.int32)
    limit_c = jnp.sum(jnp.where(one_col, cap[...], 0), axis=1, keepdims=True)
    block_c = jnp.sum(
        jnp.where(one_col, block_of(iota((1, experts), 1)), 0), axis=1, keepdims=True
    )
    key_c = jnp.where(rank_c < limit_c, slot_of(block_c, rank_c), -1)
    for c in range(CHUNKS):
        sel[c] = (iota((toks, SLOTS), 1) + c * SLOTS == key_c).astype(BF16)

    r_full = router[...]
    r_hi = r_full.astype(BF16)
    r_lo = (r_full - r_hi.astype(F32)).astype(BF16)
    group = 7 * images
    for g in range(toks // group):
        span = slice(g * group, (g + 1) * group)
        h = normed(ordered[span, :].astype(F32))
        h_hi = h.astype(BF16)
        h_lo = (h - h_hi.astype(F32)).astype(BF16)
        logits = product(h_hi, r_lo) + product(h_lo, r_hi) + product(h_hi, r_hi)
        score = jnp.sum(logits * ones_c[span], axis=1, keepdims=True)
        gate[span, :] = jnp.broadcast_to(1.0 / (1.0 + jnp.exp(-score)), (group, LANES))

    step = 1024
    last = hidden - step

    def enter(f, ref):
        ref[...] = jnp.dot(rows[...], w1[:, f : f + step], preferred_element_type=F32)

    def bend(f, ref):
        v = ref[...] + b_in[:, f : f + step]
        inner = v * (0.7978845608028654 + 0.035677408136300125 * (v * v))
        half_v = 0.5 * v
        act[:, f : f + step] = (half_v + half_v * jnp.tanh(inner)).astype(BF16)

    load1.wait()
    load2.wait()

    @pl.loop(0, CHUNKS)
    def _(c):
        each(c, lambda i: out_copy(i).wait_recv())
        take(got, c * CHUNK)
        for g in range(SLOTS // CHUNK):
            span = slice(g * CHUNK, (g + 1) * CHUNK)
            rows[span, :] = normed(rows[span, :].astype(F32)).astype(BF16)
        spare = (even, odd)
        enter(0, even)
        for n in range(1, hidden // step):
            enter(n * step, spare[n % 2])
            bend((n - 1) * step, spare[(n - 1) % 2])
        y = jnp.dot(act[:, :last], w2[:last, :], preferred_element_type=F32)
        bend(last, spare[(hidden // step - 1) % 2])
        y = y + jnp.dot(act[:, last:], w2[last:, :], preferred_element_type=F32)
        put(made, c * CHUNK, y + b_out[...])
        each(c, lambda i: back_copy(i).start())

        @pl.when(c == 0)
        def _():
            back[0] = made[0]

        @pl.when(c >= 2)
        def _():
            each(c - 2, lambda i: back_copy(i).wait_recv())
            take(back, (c - 2) * CHUNK)
            total[...] += jnp.dot(sel[c - 2], rows[...], preferred_element_type=F32)

    @pl.loop(1, PARTNERS)
    def _(i):
        out_copy(i).wait_send()

    c = CHUNKS - 2
    each(c, lambda i: back_copy(i).wait_recv())
    take(back, c * CHUNK)
    total[...] += jnp.dot(sel[c], rows[...], preferred_element_type=F32)
    c = CHUNKS - 1
    each(c, lambda i: back_copy(i).wait_recv())
    take(back, c * CHUNK)
    wide = width // 2
    for n in range(2):
        cols = slice(n * wide, (n + 1) * wide)
        part = total[:, cols] + jnp.dot(sel[c], rows[:, cols], preferred_element_type=F32)
        out[:, cols] = (ordered[:, cols].astype(F32) + gate[:, :1] * part).astype(BF16)

    @pl.loop(1, PARTNERS)
    def _(i):
        back_copy(i).wait_send()


def finish_kernel(src, out, sem):
    size = src.shape[0] // sem.shape[0]
    stores = [
        pltpu.make_async_copy(src.at[pl.ds(n * size, size)], out.at[pl.ds(n * size, size)], sem.at[n])
        for n in range(sem.shape[0])
    ]
    for copy in stores:
        copy.start()
    for copy in stores:
        copy.wait()


def per_device(
    patches, visible, routes, expert_cap, norm_gain, norm_bias, router, w_in, b_in, w_out, b_out
):
    images, _, width = patches.shape
    toks = images * visible.shape[1]
    experts = expert_cap.shape[0]
    hidden = w_in.shape[2]
    by_patch = jnp.transpose(patches, (1, 0, 2))
    vmem = pl.BlockSpec(memory_space=pltpu.VMEM)
    any_ = pl.BlockSpec(memory_space=pl.ANY)
    blk = (experts, 8, 2 * width + 3 * LANES)
    dma = pltpu.SemaphoreType.DMA
    done = jax.ShapeDtypeStruct((toks, width), BF16)
    result = pl.pallas_call(
        layer_kernel,
        out_shape=pltpu.VMEM((toks, width), BF16),
        in_specs=[any_] * 11,
        out_specs=vmem,
        scratch_shapes=[
            pltpu.VMEM(by_patch.shape[:2] + (width // 2,), BF16),
            pltpu.VMEM(by_patch.shape[:2] + (width // 2,), BF16),
            pltpu.SMEM(visible.shape, jnp.int32),
            pltpu.VMEM((1, toks), jnp.int32),
            pltpu.VMEM((1, experts), jnp.int32),
            pltpu.VMEM((1, width), F32),
            pltpu.VMEM((1, width), F32),
            pltpu.VMEM((experts, width), F32),
            pltpu.VMEM((1, hidden), F32),
            pltpu.VMEM((1, width), F32),
            pltpu.VMEM(blk, BF16),
            pltpu.VMEM(blk, BF16),
            pltpu.VMEM(blk, BF16),
            pltpu.VMEM(blk, BF16),
            pltpu.VMEM((width, hidden), BF16),
            pltpu.VMEM((hidden, width), BF16),
            pltpu.VMEM((SLOTS, width), BF16),
            pltpu.VMEM((SLOTS, hidden), BF16),
            pltpu.VMEM((SLOTS, 1024), F32),
            pltpu.VMEM((SLOTS, 1024), F32),
            pltpu.VMEM((3, 8 * CHUNK, LANES), F32),
            pltpu.VMEM((toks, width), BF16),
            pltpu.VMEM((toks, width), BF16),
            pltpu.VMEM((toks, LANES), F32),
            pltpu.VMEM((CHUNKS, toks, SLOTS), BF16),
            pltpu.VMEM((toks, width), F32),
            dma((12,)),
            dma((experts,)),
            dma((experts,)),
            dma((experts,)),
            dma((experts,)),
        ],
        compiler_params=pltpu.CompilerParams(
            collective_id=0, has_side_effects=True, vmem_limit_bytes=58 * 2**20
        ),
        name="layer",
    )(
        by_patch, visible, routes.reshape(1, toks), expert_cap.reshape(1, experts),
        norm_gain.reshape(1, width), norm_bias.reshape(1, width), router.T, w_in, b_in, w_out, b_out,
    )
    pieces = 2
    return pl.pallas_call(
        finish_kernel,
        out_shape=done,
        in_specs=[vmem],
        out_specs=any_,
        scratch_shapes=[dma((pieces,))],
        compiler_params=pltpu.CompilerParams(vmem_limit_bytes=4 * 2**20),
        name="finish",
    )(result)


def solution(mesh):
    return jax.shard_map(
        per_device,
        mesh=mesh,
        in_specs=(
            P(("dp", "expert"), None, None),
            P(("dp", "expert"), None),
            P(("dp", "expert"), None),
            P("dp"),
            P(),
            P(),
            P(),
            P("expert", None, None),
            P("expert", None),
            P("expert", None, None),
            P("expert", None),
        ),
        out_specs=P(("dp", "expert"), None),
        check_vma=False,
    )
```
